128 devices in a mesh: dp: 16 (over y_hi, z, core), vocab: 8 (over x, y_lo).
Axes of the slice: x: 4, y: 4 (y_hi: 2, y_lo: 2; y = y_hi * 2 + y_lo), z: 4, core: 2. Of those that a mesh axis runs over, the one named last changes fastest.
Arguments:
- hidden: bfloat16 [768, 5120], P('dp')
- head_weight: bfloat16 [131072, 5120], P(('dp', 'vocab'))
- target_ids: int32 [768], P('dp'), may hold values from 0 to 131071
- response_mask: int32 [768], P('dp'), may hold values 0 or 1
- advantages: bfloat16 [768], P('dp'), may hold values from -0.23925781 to 0.23925781
- seq_tokens: int32 [128], P('dp'), may hold values from 24 to 144
- layer_grads: float32 [16, 1024, 8192], P('dp', None, 'vocab'), may hold values from -3 to 3
Outputs:
- grad_hidden: bfloat16 [768, 5120], P('dp', 'vocab')
- grad_weight: bfloat16 [131072, 5120], P(('dp', 'vocab'))
- reduced_bucket: float32 [1024, 8192], P('dp', 'vocab')
The draws below stay inside these ranges and needn't reach their ends.
All inputs are finite; a program needn't handle non-finite values. No bound on the sum of `response_mask` on one device may be relied on, other than what follows from the above.
Results may differ from the reference program's by a relative error of at most 0.015.
Values may be sent and summed in bfloat16 or wider, within the bound.
A program may use at most 192 MiB of HBM per device.

```python
import math
import jax
import jax.numpy as jnp
from jax import lax

D = 5120
VOC_DEV = 1024
TOK_DEV = 48
BK_COLS = 1024
TOKENS = 768
VOCAB = 131072
SEQS = 128
BK_ROWS = 1024
N_DP = 16
N_VOCAB = 8


def head_rows(weight_key, row_ids):

    def single_row(row_index):
        values = jax.random.normal(jax.random.fold_in(weight_key, row_index), (D,), jnp.float32)
        return jnp.clip(values, -6.0, 6.0) * (3.0 / math.sqrt(D))
    return jax.vmap(single_row)(row_ids)


def draw_head_weight(key, part):
    weight_key = jax.random.fold_in(key, 11)
    row_ids = jnp.arange(VOCAB, dtype=jnp.int32).reshape(VOCAB // VOC_DEV, VOC_DEV)
    blocks = lax.map(lambda block_ids: head_rows(weight_key, block_ids).astype(jnp.bfloat16), row_ids)
    return blocks.reshape(VOCAB, D)


def peaked_rows(key, weight_key):
    shard_count = VOCAB // VOC_DEV
    peak_count = min(shard_count, D // 8)
    peak_shards = jnp.arange(peak_count, dtype=jnp.int32) * shard_count // peak_count
    key_offset, key_height = jax.random.split(jax.random.fold_in(key, 31), 2)
    offsets = jax.random.randint(key_offset, (TOKENS, peak_count), 0, VOC_DEV, dtype=jnp.int32)
    peak_ids = peak_shards[None, :] * VOC_DEV + offsets
    heights = 9.0 + jax.random.uniform(key_height, (TOKENS, peak_count), jnp.float32, -1.0, 1.0)

    def one_token(packed):
        peak_rows, peak_height = packed
        head_block = head_rows(weight_key, peak_rows).astype(jnp.bfloat16).astype(jnp.float32)
        gram_matrix = jnp.dot(head_block, head_block.T, precision=lax.Precision.HIGHEST)
        ridge_term = 0.05 * jnp.mean(jnp.diagonal(gram_matrix))
        identity = jnp.eye(peak_count, dtype=jnp.float32)
        coefficients = jnp.linalg.solve(gram_matrix + ridge_term * identity, peak_height)
        return jnp.dot(coefficients, head_block, precision=lax.Precision.HIGHEST)
    return lax.map(one_token, (peak_ids, heights))


def draw_hidden(key, part):
    weight_key = jax.random.fold_in(key, 11)
    hidden_key = jax.random.fold_in(key, 23)
    noise = jnp.clip(jax.random.normal(hidden_key, (TOKENS, D), jnp.float32), -6.0, 6.0)
    values = peaked_rows(key, weight_key) + 0.15 * noise
    values = jnp.clip(values, -6.0, 6.0)
    return values.astype(jnp.bfloat16)


def draw_seq_tokens(key, part):
    position = jnp.arange(SEQS, dtype=jnp.int32)
    centre = TOK_DEV * (SEQS - 1 + 2 * position) // (SEQS - 1)
    key_vals, key_high, key_low = jax.random.split(jax.random.fold_in(key, 37), 3)
    counts = jax.random.randint(key_vals, (SEQS,), centre // 2, centre + 1, dtype=jnp.int32)
    half = SEQS // 2
    high_pos = jax.random.randint(key_high, (), half, SEQS, dtype=jnp.int32)
    low_pos = jax.random.randint(key_low, (), 0, half, dtype=jnp.int32)
    counts = jnp.where(position == high_pos, 3 * TOK_DEV, counts)
    counts = jnp.where(position == low_pos, TOK_DEV // 2, counts)
    return counts.astype(jnp.int32)


def touch_ends(entries, stream_key, smallest, largest):
    spot = [jax.random.randint(jax.random.fold_in(stream_key, axis), (), 0, length) for axis, length in enumerate(entries.shape)]
    widest = entries.shape.index(max(entries.shape))
    next_to = spot[:widest] + [(spot[widest] + 1) % entries.shape[widest]] + spot[widest + 1:]
    return entries.at[tuple(spot)].set(smallest).at[tuple(next_to)].set(largest)


def spiked(values, stream_key, source, target, blocks, factor):
    def block_of(dim):
        return (jnp.arange(values.shape[dim]) // (values.shape[dim] // blocks)).reshape((-1,) + (1,) * (values.ndim - 1 - dim))

    one_side = jax.random.permutation(stream_key, blocks)[block_of(target)]
    far = (block_of(target) + blocks // 2) % blocks
    return jnp.where((block_of(source) == one_side) | (block_of(source) == far), factor * values, values)


def steps_of(key, shape, shards, least, largest):
    level, own = 1.0, jax.random.fold_in(key, 6)
    for dim, shards_of in shards:
        steps = jnp.exp(jax.random.uniform(jax.random.fold_in(own, dim), (shards_of,), jnp.float32, least / len(shards), largest / len(shards)))
        level = level * jnp.repeat(steps, shape[dim] // shards_of).reshape([-1 if axis == dim else 1 for axis in range(len(shape))])
    return level


def gaussian(rng, dims, spread, reach, shards=(), held_as=jnp.bfloat16):
    entries = spread * jax.random.normal(rng, dims, jnp.float32)
    if shards:
        entries = entries * steps_of(rng, dims, shards, -0.22, 0.18)
    return jnp.clip(entries, -reach, reach).astype(held_as)


def noise_with(own_key, dims, spread, reach, cuts, heavy, kind=jnp.bfloat16):
    values = spread * jax.random.normal(own_key, dims, jnp.float32)
    if cuts:
        values = values * steps_of(own_key, dims, cuts, -0.22, 0.18)
    return jnp.clip(spiked(values, jax.random.fold_in(own_key, 3), *heavy), -reach, reach).astype(kind)


def setup_inputs(seed: int = 0) -> dict:
    key_of = jax.random.split(jax.random.key(seed), 8)
    hidden = draw_hidden(jax.random.fold_in(key_of[7], 71), 0)
    head_weight = draw_head_weight(jax.random.fold_in(key_of[7], 71), 0)
    target_ids = touch_ends(jax.random.randint(key_of[2], (TOKENS,), 0, VOCAB), jax.random.fold_in(key_of[2], 1), 0, VOCAB - 1).astype(jnp.int32)
    response_mask = touch_ends((jax.random.randint(key_of[3], (TOKENS,), 0, 4) < 3).astype(jnp.int32), jax.random.fold_in(key_of[3], 1), 0, 1)
    advantages = gaussian(key_of[4], (TOKENS,), 0.04, 0.23925781, ((0, 16),))
    seq_tokens = draw_seq_tokens(jax.random.fold_in(key_of[7], 71), 0)
    layer_grads = noise_with(key_of[6], (N_DP, BK_ROWS, BK_COLS * N_VOCAB), 0.25, 3.0, ((0, 16), (2, 8)), (0, 1, 16, 2.0), jnp.float32)
    return {"hidden": hidden, "head_weight": head_weight, "target_ids": target_ids, "response_mask": response_mask, "advantages": advantages, "seq_tokens": seq_tokens, "layer_grads": layer_grads}


loss_scale = 16.0
entropy_coef = 0.1

def combine_stats(first, second):
    first_max, first_sum, first_ent, first_tgt = first
    second_max, second_sum, second_ent, second_tgt = second
    joint_max = jnp.maximum(first_max, second_max)
    first_f = jnp.exp(first_max - joint_max)
    second_f = jnp.exp(second_max - joint_max)
    return (joint_max, first_sum * first_f + second_sum * second_f, first_ent * first_f + second_ent * second_f, first_tgt + second_tgt)

def reference(hidden, head_weight, target_ids, response_mask, advantages, seq_tokens, layer_grads):
    num_blocks = head_weight.shape[0] // VOC_DEV
    w_blocks = head_weight.reshape(num_blocks, VOC_DEV, D)
    offsets = jnp.arange(num_blocks, dtype=jnp.int32) * VOC_DEV
    local_rows = jnp.arange(VOC_DEV, dtype=jnp.int32)[:, None]

    def logits_of(w_block):
        return jnp.dot(w_block.astype(jnp.float32), hidden.T.astype(jnp.float32), preferred_element_type=jnp.float32)

    def stats_step(running, packed):
        w_block, offset = packed
        logits = logits_of(w_block)
        block_max = jnp.max(logits, axis=0)
        shifted = jnp.exp(logits - block_max[None, :])
        onehot = offset + local_rows == target_ids[None, :]
        block = (block_max, jnp.sum(shifted, axis=0), jnp.sum(shifted * logits, axis=0), jnp.sum(jnp.where(onehot, logits, jnp.zeros_like(logits)), axis=0))
        return (combine_stats(running, block), None)
    tokens = hidden.shape[0]
    start_stats = (jnp.full((tokens,), -jnp.inf, dtype=jnp.float32), jnp.zeros((tokens,), jnp.float32), jnp.zeros((tokens,), jnp.float32), jnp.zeros((tokens,), jnp.float32))
    (row_max, row_sum, row_ent, row_tgt), _ = lax.scan(stats_step, start_stats, (w_blocks, offsets))
    token_total = jnp.sum(seq_tokens.astype(jnp.float32))
    factor = loss_scale * tokens / token_total
    weights = factor * response_mask.astype(jnp.float32)
    advantage = advantages.astype(jnp.float32)
    mean_logit = row_ent / row_sum

    def grad_step(accum, packed):
        w_block, offset = packed
        logits = logits_of(w_block)
        softmax = jnp.exp(logits - row_max[None, :]) / row_sum[None, :]
        onehot = (offset + local_rows == target_ids[None, :]).astype(jnp.float32)
        logit_grad = weights[None, :] * (-advantage[None, :] * (onehot - softmax) + entropy_coef * softmax * (logits - mean_logit[None, :]))
        grad_bf = logit_grad.astype(jnp.bfloat16)
        weight_grad = jnp.dot(grad_bf.astype(jnp.float32), hidden.astype(jnp.float32), preferred_element_type=jnp.float32).astype(jnp.bfloat16)
        accum = accum + jnp.dot(grad_bf.T.astype(jnp.float32), w_block.astype(jnp.float32), preferred_element_type=jnp.float32)
        return (accum, weight_grad)
    grad_sum, weight_grads = lax.scan(grad_step, jnp.zeros((tokens, D), jnp.float32), (w_blocks, offsets))
    grad_hidden = grad_sum.astype(jnp.bfloat16)
    grad_weight = weight_grads.reshape(head_weight.shape[0], D)
    reduced_bucket = jnp.sum(layer_grads, axis=0) * factor
    return (grad_hidden, grad_weight, reduced_bucket)
```

```python
import functools

import jax
import jax.numpy as jnp
from jax import lax
from jax.experimental import pallas as pl
from jax.experimental.pallas import tpu as pltpu
from jax.sharding import Mesh
from jax.sharding import PartitionSpec as P

VOCAB = ("vocab_0", "vocab_1")
DP = ("dp_0", "dp_1", "dp_2")
DP_VOCAB = ("dp_0", "dp_1", "dp_2", "vocab_0", "vocab_1")
BF, F32 = jnp.bfloat16, jnp.float32

loss_scale = 16.0
entropy_coef = 0.1

COPIES = 170


def rem4(v):
    return lax.rem(v, 4)


class Net:
    def __init__(self, send_sems, recv_sems):
        self.send_sems, self.recv_sems, self.all = send_sems, recv_sems, []

    def copy(self, src, dst, dev):
        i = len(self.all)
        c = pltpu.make_async_remote_copy(
            src_ref=src,
            dst_ref=dst,
            send_sem=self.send_sems.at[i],
            recv_sem=self.recv_sems.at[i],
            device_id=dev,
            device_id_type=pl.DeviceIdType.MESH,
        )
        c.start()
        self.all.append(c)
        return c


class Ring4:
    def __init__(self, net, me, to, chunk, recv):
        self.net, self.me, self.to, self.chunk, self.recv = net, me, to, chunk, recv

    def far(self):
        t = rem4(self.me + 2)
        self.c1 = self.net.copy(self.chunk(t, 0), self.recv.at[0, 0], self.to(1))
        self.c2 = self.net.copy(self.chunk(t, 1), self.recv.at[1, 0], self.to(3))

    def near(self):
        self.c3 = self.net.copy(self.chunk(rem4(self.me + 1), 1), self.recv.at[0, 1], self.to(1))
        self.c4 = self.net.copy(self.chunk(rem4(self.me + 3), 0), self.recv.at[1, 1], self.to(3))

    def relay(self):
        d = self.chunk(rem4(self.me + 1), 0)
        self.c1.wait_recv()
        d[...] = (d[...].astype(F32) + self.recv[0, 0].astype(F32)).astype(BF)
        self.c5 = self.net.copy(d, self.recv.at[0, 2], self.to(1))
        d = self.chunk(rem4(self.me + 3), 1)
        self.c2.wait_recv()
        d[...] = (d[...].astype(F32) + self.recv[1, 0].astype(F32)).astype(BF)
        self.c6 = self.net.copy(d, self.recv.at[1, 2], self.to(3))

    def finish(self, put):
        for c in (self.c3, self.c4, self.c5, self.c6):
            c.wait_recv()
        r, mine = self.recv, self.chunk
        me = rem4(self.me)
        put(0, mine(me, 0)[...].astype(F32) + r[0, 2].astype(F32) + r[1, 1].astype(F32))
        put(1, mine(me, 1)[...].astype(F32) + r[0, 1].astype(F32) + r[1, 2].astype(F32))


def kernel(
    hid, w_hbm, meta, lg, gh, gw, rb,
    h, w, logit, g, gt, own, snd, rcv, t_buf, r1, r1y, u0, u1, u2, r2, v, r3,
    st_s, st_c, st_r, stage, b_sib, b_own, b_s, b_r, b, b_rz, b_u, b_y, b_ry,
    send_sems, recv_sems, local_sems, gw_sems,
):
    yh, z, c = lax.axis_index("dp_0"), lax.axis_index("dp_1"), lax.axis_index("dp_2")
    x, yl = lax.axis_index("vocab_0"), lax.axis_index("vocab_1")
    y = 2 * yh + yl
    k = lax.rem(x + yh + yl, 2)

    def to_x(d):
        return {"vocab_0": rem4(x + d)}

    def to_z(d):
        return {"dp_1": rem4(z + d)}

    def to_y(d):
        n = rem4(y + d)
        return {"dp_0": n // 2, "vocab_1": lax.rem(n, 2)}

    y_other = {"dp_0": 1 - yh, "vocab_1": 1 - yl}
    y_same = {"vocab_1": 1 - yl}
    core = {"dp_2": 1 - c}

    net = Net(send_sems, recv_sems)

    ld_h = pltpu.make_async_copy(hid, h.at[:, c, yh, z], local_sems.at[0])
    ld_h.start()
    ld_bs = pltpu.make_async_copy(lg.at[:, :, 1 - c], b_sib, local_sems.at[1])
    ld_bs.start()
    ld_w = pltpu.make_async_copy(w_hbm, w, local_sems.at[2])
    ld_w.start()
    ld_bo = pltpu.make_async_copy(lg.at[:, :, c], b_own, local_sems.at[3])
    ld_bo.start()

    barrier = pltpu.get_barrier_semaphore()
    peers = [core] + [f(d) for f in (to_x, to_y, to_z) for d in (1, 2, 3)]
    for p in peers:
        pl.semaphore_signal(barrier, inc=1, device_id=p, device_id_type=pl.DeviceIdType.MESH)
    pl.semaphore_wait(barrier, len(peers))
    ld_h.wait()

    mine = pl.ds(pl.multiple_of(k * 2560, 128), 2560)
    other = pl.ds(pl.multiple_of((1 - k) * 2560, 128), 2560)
    lower = pl.ds(pl.multiple_of(k * 2560, 128), 1280)
    upper = pl.ds(pl.multiple_of(k * 2560 + 1280, 128), 1280)

    def piece(j, hi, zz, cols):
        return h.at[j, c, hi, zz, :, cols]

    def hop(j, hi, zz, cols, dev):
        ref = piece(j, hi, zz, cols)
        return net.copy(ref, ref, dev)

    yo, zm, zp, z2 = 1 - yh, rem4(z + 3), rem4(z + 1), rem4(z + 2)
    sides = (to_x(1), to_x(3), y_same)
    ag = [{} for _ in range(3)]
    for j in range(3):
        ag[j]["zm"] = hop(j, yh, z, mine, to_z(1))
        ag[j]["zp"] = hop(j, yh, z, mine, to_z(3))
        ag[j]["yo"] = hop(j, yh, z, mine, y_other)

    def across(j, p, hi, zz):
        ag[j]["b%d" % p] = hop(j, hi, zz, mine, sides[(p + j) % 3])

    def gather_relays(j):
        a = ag[j]
        a["zm"].wait_recv()
        a["z2l"] = hop(j, yh, zm, lower, to_z(1))
        across(j, 0, yh, zm)
        a["zp"].wait_recv()
        a["z2u"] = hop(j, yh, zp, upper, to_z(3))
        across(j, 1, yh, zp)
        a["yo"].wait_recv()
        a["zmo"] = hop(j, yo, z, mine, to_z(1))
        a["zpo"] = hop(j, yo, z, mine, to_z(3))
        across(j, 2, yo, z)
        a["z2l"].wait_recv()
        a["z2u"].wait_recv()
        a["yo2"] = hop(j, yh, z2, mine, y_other)
        across(j, 5, yh, z2)
        a["zmo"].wait_recv()
        across(j, 3, yo, zm)
        a["zpo"].wait_recv()
        across(j, 4, yo, zp)
        a["yo2"].wait_recv()
        across(j, 6, yo, z2)
        ref = h.at[j, c, :, :, :, mine]
        a["d0"] = net.copy(ref, ref, core)

    def gather_across(j):
        for p in range(7):
            ag[j]["b%d" % p].wait_recv()
        ref = h.at[j, c, :, :, :, other]
        ag[j]["d1"] = net.copy(ref, ref, core)

    def gather_done(j):
        ag[j]["d0"].wait_recv()
        ag[j]["d1"].wait_recv()

    def bucket_pair():
        ld_bs.wait()
        b_s[...] = b_sib[...].astype(BF)
        return net.copy(b_s, b_r, core)

    def bucket_sum(cp):
        ld_bo.wait()
        cp.wait_recv()
        b[...] = (b_own[...] + b_r[...].astype(F32)).astype(BF)

    bz = Ring4(net, z, to_z, lambda t, hf: b.at[hf, t], b_rz)

    def b_put(hf, val):
        b_u[hf] = val

    def logits(j, half):
        rows = pl.ds(half * 512, 512)
        hj = h[j].reshape(256, 5120)
        logit[j, rows] = lax.dot_general(
            w[rows], hj, (((1,), (1,)), ((), ())), preferred_element_type=F32
        )

    row_id = lax.broadcasted_iota(jnp.int32, (8, 256), 0)

    def local_stats(j):
        def top(i, m):
            blk = logit[j, pl.ds(pl.multiple_of(i * 128, 128), 128)]
            return jnp.maximum(m, jnp.max(blk.reshape(16, 8, 256), axis=0))

        m8 = lax.fori_loop(0, 8, top, jnp.full((8, 256), -jnp.inf, F32))
        m = jnp.max(m8, axis=0, keepdims=True)

        def sums(i, se):
            blk = logit[j, pl.ds(pl.multiple_of(i * 128, 128), 128)]
            e = jnp.exp(blk - m)
            return (
                se[0] + jnp.sum(e.reshape(16, 8, 256), axis=0),
                se[1] + jnp.sum((e * blk).reshape(16, 8, 256), axis=0),
            )

        zero = jnp.zeros((8, 256), F32)
        s8, e8 = lax.fori_loop(0, 8, sums, (zero, zero))
        s = jnp.sum(s8, axis=0, keepdims=True)
        e = jnp.sum(e8, axis=0, keepdims=True)
        tile = meta[j]
        tile = jnp.where(row_id == 0, m, tile)
        tile = jnp.where(row_id == 1, s, tile)
        tile = jnp.where(row_id == 2, e, tile)
        return tile

    phases = (
        [core],
        [to_x(d) for d in (1, 2, 3)],
        [to_y(d) for d in (1, 2, 3)],
        [to_z(d) for d in (1, 2, 3)],
    )
    st = [None] * 3

    def stats_send(j, ph, tile):
        st_s[j, ph] = tile
        st[j] = [
            net.copy(st_s.at[j, ph], st_r.at[j, ph, d], dev) for d, dev in enumerate(phases[ph])
        ]

    def stats_recv(j, ph):
        tiles = [st_s[j, ph]]
        for d, cp in enumerate(st[j]):
            cp.wait_recv()
            tiles.append(st_r[j, ph, d])
        m = functools.reduce(jnp.maximum, [t[0:1] for t in tiles])
        total = None
        for t in tiles:
            f = jnp.exp(t[0:1] - m)
            scaled = t * jnp.where((row_id == 1) | (row_id == 2), f, 1.0)
            total = scaled if total is None else total + scaled
        return jnp.where(row_id == 0, m, total)

    def stats_next(j, ph):
        stats_send(j, ph, stats_recv(j, ph - 1))

    def stats_end(j):
        st_c[j] = stats_recv(j, 3)

    def factor_of(count_row):
        return (loss_scale * 768.0) / (count_row / 8.0)

    first_id = ((yh * 8 + z * 2 + c) * 8 + x * 2 + yl) * 1024

    def grads(j):
        tile = st_c[j]
        m, s, e = tile[0:1], tile[1:2], tile[2:3]
        target = tile[3:4] / 8.0
        mask = tile[4:5] / 8.0
        adv = tile[5:6] / 8.0
        inv = 1.0 / s
        mean = e * inv
        wt = factor_of(tile[6:7]) * mask
        wa = wt * adv
        wb = wt * entropy_coef

        def block(i, _):
            rows = pl.ds(pl.multiple_of(i * 128, 128), 128)
            l = logit[j, rows]
            ids = (first_id + i * 128 + lax.broadcasted_iota(jnp.int32, (128, 256), 0)).astype(F32)
            p = jnp.exp(l - m) * inv
            val = p * (wa + wb * (l - mean))
            val = jnp.where(ids == target, val - wa, val)
            g[rows, j * 256 : (j + 1) * 256] = val.astype(BF)
            for cc in range(2):
                gt[j, (c if cc == 0 else 1 - c), :, rows] = (
                    val[:, cc * 128 : (cc + 1) * 128].T.astype(BF)
                )
            return 0

        lax.fori_loop(0, 8, block, 0)

    xs_of = [rem4(x + 2), rem4(x + 1), rem4(x + 3), x]
    pair = {}

    def terms(j, s):
        n = 4 * j + s
        cols = pl.ds(pl.multiple_of(xs_of[s] * 1280, 128), 1280)
        acc = jnp.dot(gt[j].reshape(256, 1024), w[:, cols], preferred_element_type=F32)
        for lo in range(2):
            part = acc[:, lo * 640 : (lo + 1) * 640]
            own[n % 3, lo] = part[:128].reshape(2, 4, 16, 640)
            snd[n, lo] = part[128:].reshape(2, 4, 16, 640).astype(BF)
        pair[n] = net.copy(snd.at[n], rcv.at[n], core)

    def joined(n):
        j, s = n // 4, n % 4
        pair[n].wait_recv()
        for lo in range(2):
            t_buf[j, :, :, xs_of[s], lo] = (own[n % 3, lo] + rcv[n, lo].astype(F32)).astype(BF)

    t0, t1, t2 = t_buf.at[0], t_buf.at[1], t_buf.at[2]
    rings = [
        Ring4(net, x, to_x, lambda t, hf: t0.at[hf, :, t], r1.at[0]),
        Ring4(
            net, y, to_y,
            lambda t, hf: t1.at[t // 2, 2 * hf : 2 * hf + 2, :, lax.rem(t, 2)], r1y,
        ),
        Ring4(net, z, to_z, lambda t, hf: t2.at[hf, t], r1.at[1]),
    ]
    second = [
        Ring4(
            net, y, to_y,
            lambda t, hf: u0.at[t // 2, 2 * hf : 2 * hf + 2, lax.rem(t, 2)], r2.at[0],
        ),
        Ring4(net, z, to_z, lambda t, hf: u1.at[t, 2 * hf : 2 * hf + 2], r2.at[1]),
        Ring4(net, x, to_x, lambda t, hf: u2.at[hf, t], r2.at[2]),
    ]

    def put1(j):
        def put(hf, val):
            if j == 0:
                u0[hf] = val.astype(BF)
            elif j == 1:
                u1[2 * hf : 2 * hf + 2] = val.astype(BF)
            else:
                u2[hf] = val.astype(BF)

        return put

    def put2(j):
        def put(hf, val):
            v[j, 2 * hf : 2 * hf + 2] = val.astype(BF)

        return put

    last_axis = [(z, to_z), (x, to_x), (y, to_y)]
    last = [None] * 3

    def third(j):
        me, to = last_axis[j]
        last[j] = [net.copy(v.at[j, rem4(me + d)], r3.at[j, d - 1], to(d)) for d in (1, 2, 3)]

    def rs_end(j):
        total = v[j, last_axis[j][0]].astype(F32)
        for d in range(3):
            last[j][d].wait_recv()
            total = total + r3[j, d].astype(F32)
        gh[j] = total.astype(BF)

    def rs_step(j, i):
        if i == 1:
            rings[j].relay()
        elif i == 2:
            rings[j].finish(put1(j))
            second[j].far()
            second[j].near()
        elif i == 3:
            second[j].relay()
        elif i == 4:
            second[j].finish(put2(j))
            third(j)
        elif i == 5:
            rs_end(j)

    out = {}

    def weight_grad(n):
        if n >= 2:
            out[n - 2].wait()
        cols = slice(n * 512, (n + 1) * 512)
        hn = h[:, :, :, :, :, cols].reshape(768, 512)
        stage[n % 2] = jnp.dot(g[...], hn, preferred_element_type=F32).astype(BF)
        out[n] = pltpu.make_async_copy(stage.at[n % 2], gw.at[:, cols], gw_sems.at[n])
        out[n].start()

    bp = bucket_pair()
    gather_relays(0)
    gather_relays(1)
    bucket_sum(bp)
    gather_across(0)
    gather_relays(2)
    bz.far()
    bz.near()
    ld_w.wait()
    gather_done(0)
    logits(0, 0)
    gather_across(1)
    logits(0, 1)
    stats_send(0, 0, local_stats(0))
    gather_across(2)
    bz.relay()
    gather_done(1)
    logits(1, 0)
    stats_next(0, 1)
    logits(1, 1)
    stats_next(0, 2)
    stats_send(1, 0, local_stats(1))
    gather_done(2)
    logits(2, 0)
    stats_next(0, 3)
    stats_next(1, 1)
    logits(2, 1)
    stats_next(1, 2)
    stats_send(2, 0, local_stats(2))
    stats_end(0)
    grads(0)
    stats_next(2, 1)
    stats_next(1, 3)
    terms(0, 0)
    terms(0, 1)
    stats_next(2, 2)
    stats_end(1)
    joined(0)
    rings[0].far()
    terms(0, 2)
    joined(1)
    stats_next(2, 3)
    terms(0, 3)
    joined(2)
    rings[0].near()
    grads(1)
    stats_end(2)
    joined(3)
    terms(1, 0)
    terms(1, 1)
    joined(4)
    terms(1, 2)
    joined(5)
    rs_step(0, 1)
    terms(1, 3)
    joined(6)
    grads(2)
    joined(7)
    rings[1].far()
    rings[1].near()
    terms(2, 0)
    terms(2, 1)
    joined(8)
    terms(2, 2)
    joined(9)
    terms(2, 3)
    joined(10)
    rs_step(1, 1)
    joined(11)
    rings[2].far()
    rings[2].near()

    bz.finish(b_put)
    b_y[...] = b_u[1 - yh].astype(BF)
    by = net.copy(b_y, b_ry, {"dp_0": 1 - yh})

    rs_step(0, 2)
    weight_grad(0)
    weight_grad(1)
    rs_step(0, 3)
    rs_step(1, 2)
    weight_grad(2)
    rs_step(0, 4)
    weight_grad(3)
    rs_step(2, 1)
    rs_step(1, 3)
    weight_grad(4)
    weight_grad(5)
    rs_step(1, 4)
    rs_step(0, 5)
    by.wait_recv()
    factor = factor_of(st_c[0][6:7, 0:1])
    rb[...] = (b_u[yh] + b_ry[...].astype(F32)) * factor
    weight_grad(6)
    weight_grad(7)
    rs_step(2, 2)
    rs_step(1, 5)
    weight_grad(8)
    rs_step(2, 3)
    weight_grad(9)
    rs_step(2, 4)
    rs_step(2, 5)
    out[8].wait()
    out[9].wait()
    for cp in net.all:
        cp.wait_send()


def on_device(hidden, head_weight, target_ids, response_mask, advantages, seq_tokens, layer_grads):
    yh, z, c = lax.axis_index("dp_0"), lax.axis_index("dp_1"), lax.axis_index("dp_2")
    count = jnp.sum(seq_tokens).astype(F32)
    rows = jnp.stack(
        [target_ids.astype(F32), response_mask.astype(F32), advantages.astype(F32)]
    ).reshape(3, 3, 16)
    lane = jnp.arange(256, dtype=jnp.int32)
    place = lane // 16 == c * 8 + yh * 4 + z
    spread = jnp.where(place[None, None, :], jnp.tile(rows, (1, 1, 16)), 0.0)
    meta = jnp.concatenate(
        [
            jnp.zeros((3, 3, 256), F32),
            jnp.transpose(spread, (1, 0, 2)),
            jnp.full((3, 1, 256), count, F32),
            jnp.zeros((3, 1, 256), F32),
        ],
        axis=1,
    )
    vm = pltpu.VMEM
    anywhere = pl.BlockSpec(memory_space=pl.ANY)
    in_vmem = pl.BlockSpec(memory_space=pltpu.VMEM)
    piece = (16, 640)
    scratch = [
        vm((3, 2, 2, 4, 16, 5120), BF),
        vm((1024, 5120), BF),
        vm((3, 1024, 256), F32),
        vm((1024, 768), BF),
        vm((3, 2, 128, 1024), BF),
        vm((3, 2, 2, 4, *piece), F32),
        vm((12, 2, 2, 4, *piece), BF),
        vm((12, 2, 2, 4, *piece), BF),
        vm((3, 2, 4, 4, 2, *piece), BF),
        vm((2, 2, 3, 4, 2, *piece), BF),
        vm((2, 3, 2, 4, *piece), BF),
        vm((2, 4, 2, *piece), BF),
        vm((4, 4, *piece), BF),
        vm((2, 4, 2, *piece), BF),
        vm((3, 2, 3, 2, *piece), BF),
        vm((3, 4, *piece), BF),
        vm((3, 3, *piece), BF),
        vm((3, 4, 8, 256), F32),
        vm((3, 8, 256), F32),
        vm((3, 4, 3, 8, 256), F32),
        vm((2, 1024, 512), BF),
        vm((2, 4, 64, 1024), F32),
        vm((2, 4, 64, 1024), F32),
        vm((2, 4, 64, 1024), BF),
        vm((2, 4, 64, 1024), BF),
        vm((2, 4, 64, 1024), BF),
        vm((2, 3, 64, 1024), BF),
        vm((2, 64, 1024), F32),
        vm((64, 1024), BF),
        vm((64, 1024), BF),
        pltpu.SemaphoreType.DMA((COPIES,)),
        pltpu.SemaphoreType.DMA((COPIES,)),
        pltpu.SemaphoreType.DMA((4,)),
        pltpu.SemaphoreType.DMA((10,)),
    ]
    gh, gw, rb = pl.pallas_call(
        kernel,
        out_shape=(
            jax.ShapeDtypeStruct((3, 16, 640), BF),
            jax.ShapeDtypeStruct((1024, 5120), BF),
            jax.ShapeDtypeStruct((64, 1024), F32),
        ),
        in_specs=[anywhere, anywhere, in_vmem, anywhere],
        out_specs=(in_vmem, anywhere, in_vmem),
        scratch_shapes=scratch,
        compiler_params=pltpu.CompilerParams(
            collective_id=0, has_side_effects=True, vmem_limit_bytes=67043328
        ),
    )(
        hidden.reshape(3, 16, 5120),
        head_weight,
        meta,
        layer_grads.reshape(2, 4, 2, 64, 1024),
    )
    return gh.reshape(48, 640), gw, rb


def solution(mesh):
    split = Mesh(
        mesh.devices.reshape(2, 4, 2, 4, 2), ("dp_0", "dp_1", "dp_2", "vocab_0", "vocab_1")
    )
    return jax.shard_map(
        on_device,
        mesh=split,
        in_specs=(P(DP, None), P(DP_VOCAB, None), P(DP), P(DP), P(DP), P(DP), P(DP, None, VOCAB)),
        out_specs=(P(DP, VOCAB), P(DP_VOCAB, None), P(DP, VOCAB)),
        check_vma=False,
    )
```

```python
import functools

import jax
import jax.numpy as jnp
from jax import lax
from jax.experimental import pallas as pl
from jax.experimental.pallas import tpu as pltpu
from jax.sharding import Mesh
from jax.sharding import PartitionSpec as P

VOCAB = ("vocab_0", "vocab_1")
DP = ("dp_0", "dp_1", "dp_2")
DP_VOCAB = ("dp_0", "dp_1", "dp_2", "vocab_0", "vocab_1")
BF, F32 = jnp.bfloat16, jnp.float32

loss_scale = 16.0
entropy_coef = 0.1

COPIES = 156


def rem4(v):
    return lax.rem(v, 4)


class Net:
    def __init__(self, send_sems, recv_sems):
        self.send_sems, self.recv_sems, self.all = send_sems, recv_sems, []

    def copy(self, src, dst, dev):
        i = len(self.all)
        c = pltpu.make_async_remote_copy(
            src_ref=src,
            dst_ref=dst,
            send_sem=self.send_sems.at[i],
            recv_sem=self.recv_sems.at[i],
            device_id=dev,
            device_id_type=pl.DeviceIdType.MESH,
        )
        c.start()
        self.all.append(c)
        return c


class Ring4:
    def __init__(self, net, me, to, chunk, recv):
        self.net, self.me, self.to, self.chunk, self.recv = net, me, to, chunk, recv

    def far(self):
        t = rem4(self.me + 2)
        self.c1 = self.net.copy(self.chunk(t, 0), self.recv.at[0, 0], self.to(1))
        self.c2 = self.net.copy(self.chunk(t, 1), self.recv.at[1, 0], self.to(3))

    def near(self):
        self.c3 = self.net.copy(self.chunk(rem4(self.me + 1), 1), self.recv.at[0, 1], self.to(1))
        self.c4 = self.net.copy(self.chunk(rem4(self.me + 3), 0), self.recv.at[1, 1], self.to(3))

    def relay(self):
        d = self.chunk(rem4(self.me + 1), 0)
        self.c1.wait_recv()
        d[...] = (d[...].astype(F32) + self.recv[0, 0].astype(F32)).astype(BF)
        self.c5 = self.net.copy(d, self.recv.at[0, 2], self.to(1))
        d = self.chunk(rem4(self.me + 3), 1)
        self.c2.wait_recv()
        d[...] = (d[...].astype(F32) + self.recv[1, 0].astype(F32)).astype(BF)
        self.c6 = self.net.copy(d, self.recv.at[1, 2], self.to(3))

    def finish(self, put):
        for c in (self.c3, self.c4, self.c5, self.c6):
            c.wait_recv()
        r, mine = self.recv, self.chunk
        me = rem4(self.me)
        put(0, mine(me, 0)[...].astype(F32) + r[0, 2].astype(F32) + r[1, 1].astype(F32))
        put(1, mine(me, 1)[...].astype(F32) + r[0, 1].astype(F32) + r[1, 2].astype(F32))


def kernel(
    hid, w_hbm, tgt, msk, adv, seq, lg, w, gh, rb,
    g, h, logit, gt, own, snd, rcv, t_buf, r1, r1y, r1z, u0, u1, u2, r2, v, r3,
    st_s, st_c, st_r, b_sib, b_own, b_s, b_r, b, b_rz, b_u, b_y, b_ry,
    send_sems, recv_sems, local_sems,
):
    yh, z, c = lax.axis_index("dp_0"), lax.axis_index("dp_1"), lax.axis_index("dp_2")
    x, yl = lax.axis_index("vocab_0"), lax.axis_index("vocab_1")
    y = 2 * yh + yl
    k = lax.rem(x + yh + yl, 2)

    def to_x(d):
        return {"vocab_0": rem4(x + d)}

    def to_z(d):
        return {"dp_1": rem4(z + d)}

    def to_y(d):
        n = rem4(y + d)
        return {"dp_0": n // 2, "vocab_1": lax.rem(n, 2)}

    y_other = {"dp_0": 1 - yh, "vocab_1": 1 - yl}
    y_same = {"vocab_1": 1 - yl}
    core = {"dp_2": 1 - c}

    net = Net(send_sems, recv_sems)

    ld_h = pltpu.make_async_copy(hid, h.at[:, c, yh, z], local_sems.at[0])
    ld_h.start()
    ld_bs = pltpu.make_async_copy(lg.at[:, :, 1 - c], b_sib, local_sems.at[1])
    ld_bs.start()
    ld_w = pltpu.make_async_copy(w_hbm, w, local_sems.at[2])
    ld_w.start()
    ld_bo = pltpu.make_async_copy(lg.at[:, :, c], b_own, local_sems.at[3])
    ld_bo.start()

    barrier = pltpu.get_barrier_semaphore()
    peers = [core] + [f(d) for f in (to_x, to_y, to_z) for d in (1, 2, 3)]
    for p in peers:
        pl.semaphore_signal(barrier, inc=1, device_id=p, device_id_type=pl.DeviceIdType.MESH)
    pl.semaphore_wait(barrier, len(peers))
    ld_h.wait()

    mine = pl.ds(pl.multiple_of(k * 2560, 128), 2560)
    other = pl.ds(pl.multiple_of((1 - k) * 2560, 128), 2560)
    lower = pl.ds(pl.multiple_of(k * 2560, 128), 1280)
    upper = pl.ds(pl.multiple_of(k * 2560 + 1280, 128), 1280)

    def piece(j, hi, zz, cols):
        return h.at[j, c, hi, zz, :, cols]

    def hop(j, hi, zz, cols, dev):
        ref = piece(j, hi, zz, cols)
        return net.copy(ref, ref, dev)

    yo, zm, zp, z2 = 1 - yh, rem4(z + 3), rem4(z + 1), rem4(z + 2)
    sides = (to_x(1), to_x(3), y_same)
    ag = [{} for _ in range(3)]
    for j in range(3):
        ag[j]["zm"] = hop(j, yh, z, mine, to_z(1))
        ag[j]["zp"] = hop(j, yh, z, mine, to_z(3))
        ag[j]["yo"] = hop(j, yh, z, mine, y_other)

    def across(j, p, hi, zz):
        ag[j]["b%d" % p] = hop(j, hi, zz, mine, sides[(p + j) % 3])

    def relay_near(j):
        a = ag[j]
        a["zm"].wait_recv()
        a["z2l"] = hop(j, yh, zm, lower, to_z(1))
        across(j, 0, yh, zm)
        a["zp"].wait_recv()
        a["z2u"] = hop(j, yh, zp, upper, to_z(3))
        across(j, 1, yh, zp)

    def relay_other(j):
        a = ag[j]
        a["yo"].wait_recv()
        a["zmo"] = hop(j, yo, z, mine, to_z(1))
        a["zpo"] = hop(j, yo, z, mine, to_z(3))
        across(j, 2, yo, z)

    def relay_far(j):
        a = ag[j]
        a["z2l"].wait_recv()
        a["z2u"].wait_recv()
        a["yo2"] = hop(j, yh, z2, mine, y_other)
        across(j, 5, yh, z2)

    def relay_last(j):
        a = ag[j]
        a["zmo"].wait_recv()
        across(j, 3, yo, zm)
        a["zpo"].wait_recv()
        across(j, 4, yo, zp)

    def relay_end(j):
        a = ag[j]
        a["yo2"].wait_recv()
        across(j, 6, yo, z2)
        ref = h.at[j, c, :, :, :, mine]
        a["d0"] = net.copy(ref, ref, core)

    def gather_across(j):
        for p in range(7):
            ag[j]["b%d" % p].wait_recv()
        ref = h.at[j, c, :, :, :, other]
        ag[j]["d1"] = net.copy(ref, ref, core)

    def gather_done(j):
        ag[j]["d0"].wait_recv()
        ag[j]["d1"].wait_recv()

    def bucket_pair():
        ld_bs.wait()
        b_s[...] = b_sib[...].astype(BF)
        return net.copy(b_s, b_r, core)

    def bucket_sum(cp):
        ld_bo.wait()
        cp.wait_recv()
        b[...] = (b_own[...] + b_r[...].astype(F32)).astype(BF)

    bz = Ring4(net, z, to_z, lambda t, hf: b.at[hf, t], b_rz)

    def b_put(hf, val):
        b_u[hf] = val

    def logits():
        def block(i, _):
            rows = pl.ds(pl.multiple_of(i * 512, 512), 512)
            logit[rows] = lax.dot_general(
                w[rows], h[...].reshape(768, 5120), (((1,), (1,)), ((), ())),
                preferred_element_type=F32,
            )
            return 0

        lax.fori_loop(0, 2, block, 0)

    def place_meta():
        r8 = lax.broadcasted_iota(jnp.int32, (8, 48), 0)
        rows = jnp.zeros((8, 48), F32)
        for r, ref in enumerate((tgt, msk, adv)):
            rows = jnp.where(r8 == r, ref[...].astype(F32).reshape(1, 48), rows)
        count = jnp.sum(seq[...].astype(F32).reshape(1, 8), axis=1, keepdims=True)
        token = lax.broadcasted_iota(jnp.int32, (48, 256), 0)
        lane = lax.broadcasted_iota(jnp.int32, (48, 256), 1)
        base = (c * 8 + yh * 4 + z) * 16
        for j in range(3):
            hot = jnp.where(lane - base == token - 16 * j, 1.0, 0.0)
            hot = jnp.where((token >= 16 * j) & (token < 16 * j + 16), hot, 0.0)
            put = lax.dot_general(
                rows, hot, (((1,), (0,)), ((), ())),
                preferred_element_type=F32, precision=lax.Precision.HIGHEST,
            )
            r_id = lax.broadcasted_iota(jnp.int32, (8, 256), 0)
            tile = jnp.where(r_id == 6, count, 0.0)
            for r in range(3):
                tile = jnp.where(r_id == 3 + r, put[r : r + 1], tile)
            st_c[:, j * 256 : (j + 1) * 256] = tile

    row_id = lax.broadcasted_iota(jnp.int32, (8, 768), 0)

    def local_stats():
        def top(i, m):
            blk = logit[pl.ds(pl.multiple_of(i * 64, 64), 64)]
            return jnp.maximum(m, jnp.max(blk.reshape(8, 8, 768), axis=0))

        m8 = lax.fori_loop(0, 16, top, jnp.full((8, 768), -jnp.inf, F32))
        m = jnp.max(m8, axis=0, keepdims=True)

        def sums(i, se):
            blk = logit[pl.ds(pl.multiple_of(i * 64, 64), 64)]
            e = jnp.exp(blk - m)
            return (
                se[0] + jnp.sum(e.reshape(8, 8, 768), axis=0),
                se[1] + jnp.sum((e * blk).reshape(8, 8, 768), axis=0),
            )

        zero = jnp.zeros((8, 768), F32)
        s8, e8 = lax.fori_loop(0, 16, sums, (zero, zero))
        s = jnp.sum(s8, axis=0, keepdims=True)
        e = jnp.sum(e8, axis=0, keepdims=True)
        tile = st_c[...]
        tile = jnp.where(row_id == 0, m, tile)
        tile = jnp.where(row_id == 1, s, tile)
        tile = jnp.where(row_id == 2, e, tile)
        return tile

    phases = (
        [core],
        [to_x(d) for d in (1, 2, 3)],
        [to_y(d) for d in (1, 2, 3)],
        [to_z(d) for d in (1, 2, 3)],
    )
    st = {}

    def stats_send(ph, tile):
        st_s[ph] = tile
        st[ph] = [net.copy(st_s.at[ph], st_r.at[ph, d], dev) for d, dev in enumerate(phases[ph])]

    def stats_recv(ph):
        tiles = [st_s[ph]]
        for d, cp in enumerate(st[ph]):
            cp.wait_recv()
            tiles.append(st_r[ph, d])
        m = functools.reduce(jnp.maximum, [t[0:1] for t in tiles])
        total = None
        for t in tiles:
            f = jnp.exp(t[0:1] - m)
            scaled = t * jnp.where((row_id == 1) | (row_id == 2), f, 1.0)
            total = scaled if total is None else total + scaled
        return jnp.where(row_id == 0, m, total)

    def stats_next(ph):
        stats_send(ph, stats_recv(ph - 1))

    def stats_end():
        st_c[...] = stats_recv(3)

    def factor_of(count_row):
        return (loss_scale * 768.0) / (count_row / 8.0)

    first_id = ((yh * 8 + z * 2 + c) * 8 + x * 2 + yl) * 1024

    def grads():
        tile = st_c[...]
        m, s, e = tile[0:1], tile[1:2], tile[2:3]
        target = tile[3:4] / 8.0
        mask = tile[4:5] / 8.0
        adv = tile[5:6] / 8.0
        inv = 1.0 / s
        mean = e * inv
        wt = factor_of(tile[6:7]) * mask
        wa = wt * adv
        wb = wt * entropy_coef

        def block(i, _):
            rows = pl.ds(pl.multiple_of(i * 128, 128), 128)
            l = logit[rows]
            ids = (first_id + i * 128 + lax.broadcasted_iota(jnp.int32, (128, 768), 0)).astype(F32)
            p = jnp.exp(l - m) * inv
            val = p * (wa + wb * (l - mean))
            val = jnp.where(ids == target, val - wa, val)
            g[rows] = val.astype(BF)
            for j in range(3):
                for cc in range(2):
                    at = (2 * j + cc) * 128
                    gt[(c if cc == 0 else 1 - c), j, :, rows] = val[:, at : at + 128].T.astype(BF)
            return 0

        lax.fori_loop(0, 8, block, 0)

    xs_of = [rem4(x + 2), rem4(x + 1), rem4(x + 3), x]
    pair = {}

    def terms(s):
        cols = pl.ds(pl.multiple_of(xs_of[s] * 1280, 128), 1280)
        acc = jnp.dot(gt[...].reshape(768, 1024), w[:, cols], preferred_element_type=F32)
        for lo in range(2):
            part = acc[:, lo * 640 : (lo + 1) * 640]
            own[s % 2, lo] = part[:384].reshape(3, 2, 4, 16, 640)
            snd[s, lo] = part[384:].reshape(3, 2, 4, 16, 640).astype(BF)
        pair[s] = net.copy(snd.at[s], rcv.at[s], core)

    def joined(s):
        pair[s].wait_recv()
        for lo in range(2):
            t_buf[:, :, :, xs_of[s], lo] = (own[s % 2, lo] + rcv[s, lo].astype(F32)).astype(BF)

    t0, t1, t2 = t_buf.at[0], t_buf.at[1], t_buf.at[2]
    ring_x = Ring4(net, x, to_x, lambda t, hf: t0.at[hf, :, t], r1)
    ring_y, ring_z = [], []
    for s in range(4):
        ring_y.append(
            Ring4(
                net, y, to_y,
                lambda t, hf, s=s: t1.at[t // 2, 2 * hf : 2 * hf + 2, xs_of[s], lax.rem(t, 2)],
                r1y.at[s],
            )
        )
        ring_z.append(Ring4(net, z, to_z, lambda t, hf, s=s: t2.at[hf, t, xs_of[s]], r1z.at[s]))

    def put_x(hf, val):
        u0[hf] = val.astype(BF)

    def put_y(s):
        def put(hf, val):
            u1[2 * hf : 2 * hf + 2, xs_of[s]] = val.astype(BF)

        return put

    def put_z(s):
        def put(hf, val):
            u2[hf, xs_of[s]] = val.astype(BF)

        return put

    def start(s):
        for r in (ring_y[s], ring_z[s]):
            r.far()
            r.near()

    def relay(s):
        ring_y[s].relay()
        ring_z[s].relay()

    def finish(s):
        ring_y[s].finish(put_y(s))
        ring_z[s].finish(put_z(s))

    def begin_second(j):
        second[j].far()
        second[j].near()

    second = [
        Ring4(
            net, y, to_y,
            lambda t, hf: u0.at[t // 2, 2 * hf : 2 * hf + 2, lax.rem(t, 2)], r2.at[0],
        ),
        Ring4(net, z, to_z, lambda t, hf: u1.at[t, 2 * hf : 2 * hf + 2], r2.at[1]),
        Ring4(net, x, to_x, lambda t, hf: u2.at[hf, t], r2.at[2]),
    ]

    def put2(j):
        def put(hf, val):
            v[j, 2 * hf : 2 * hf + 2] = val.astype(BF)

        return put

    last_axis = [(z, to_z), (x, to_x), (y, to_y)]
    last = [None] * 3

    def third(j):
        me, to = last_axis[j]
        last[j] = [net.copy(v.at[j, rem4(me + d)], r3.at[j, d - 1], to(d)) for d in (1, 2, 3)]

    def rs_end(j):
        total = v[j, last_axis[j][0]].astype(F32)
        for d in range(3):
            last[j][d].wait_recv()
            total = total + r3[j, d].astype(F32)
        gh[j] = total.astype(BF)

    def end_second(j):
        second[j].finish(put2(j))
        third(j)

    def weight_grad(n):
        cols = slice(n * 512, (n + 1) * 512)
        hn = h[:, :, :, :, :, cols].reshape(768, 512)
        w[:, cols] = jnp.dot(g[...], hn, preferred_element_type=F32).astype(BF)

    bp = bucket_pair()
    place_meta()
    relay_near(0)
    relay_other(0)
    relay_near(1)
    relay_other(1)
    relay_near(2)
    relay_far(0)
    relay_other(2)
    relay_far(1)
    relay_last(0)
    relay_far(2)
    relay_end(0)
    relay_last(1)
    relay_end(1)
    bucket_sum(bp)
    relay_last(2)
    relay_end(2)
    bz.far()
    bz.near()
    ld_w.wait()
    gather_across(0)
    gather_across(1)
    gather_across(2)
    bz.relay()
    gather_done(0)
    gather_done(1)
    gather_done(2)
    logits()
    stats_send(0, local_stats())
    bz.finish(b_put)
    stats_next(1)
    b_y[...] = b_u[1 - yh].astype(BF)
    stats_next(2)
    stats_next(3)
    stats_end()
    grads()
    terms(0)
    terms(1)
    joined(0)
    ring_x.far()
    start(0)
    terms(2)
    joined(1)
    start(1)
    relay(0)
    terms(3)
    joined(2)
    ring_x.near()
    start(2)
    relay(1)
    ring_x.relay()
    joined(3)
    start(3)
    weight_grad(0)
    weight_grad(1)
    relay(2)
    finish(0)
    weight_grad(2)
    weight_grad(3)
    relay(3)
    finish(1)
    ring_x.finish(put_x)
    begin_second(0)
    weight_grad(4)
    finish(2)
    weight_grad(5)
    finish(3)
    begin_second(1)
    begin_second(2)
    second[0].relay()
    by = net.copy(b_y, b_ry, {"dp_0": 1 - yh})
    weight_grad(6)
    second[1].relay()
    second[2].relay()
    end_second(0)
    weight_grad(7)
    end_second(1)
    end_second(2)
    weight_grad(8)
    by.wait_recv()
    rb[...] = (b_u[yh] + b_ry[...].astype(F32)) * factor_of(st_c[6:7, 0:1])
    weight_grad(9)
    for j in range(3):
        rs_end(j)
    for cp in net.all:
        cp.wait_send()


def flush(gw_in, gh_in, rb_in, gh, gw, rb, sems):
    copies = [
        pltpu.make_async_copy(gw_in.at[rows], gw.at[rows], sems.at[i])
        for i, rows in enumerate(pl.ds(128 * k, 128) for k in range(8))
    ]
    copies.append(pltpu.make_async_copy(gh_in, gh, sems.at[8]))
    copies.append(pltpu.make_async_copy(rb_in, rb, sems.at[9]))
    for cp in copies:
        cp.start()
    for cp in copies:
        cp.wait()


def on_device(hidden, head_weight, target_ids, response_mask, advantages, seq_tokens, layer_grads):
    vm = pltpu.VMEM
    anywhere = pl.BlockSpec(memory_space=pl.ANY)
    in_vmem = pl.BlockSpec(memory_space=pltpu.VMEM)
    piece = (16, 640)
    scratch = [
        vm((1024, 768), BF),
        vm((3, 2, 2, 4, 16, 5120), BF),
        vm((1024, 768), F32),
        vm((2, 3, 128, 1024), BF),
        vm((2, 2, 3, 2, 4, *piece), F32),
        vm((4, 2, 3, 2, 4, *piece), BF),
        vm((4, 2, 3, 2, 4, *piece), BF),
        vm((3, 2, 4, 4, 2, *piece), BF),
        vm((2, 3, 4, 2, *piece), BF),
        vm((4, 2, 3, 2, *piece), BF),
        vm((4, 2, 3, 2, *piece), BF),
        vm((2, 4, 2, *piece), BF),
        vm((4, 4, *piece), BF),
        vm((2, 4, 2, *piece), BF),
        vm((3, 2, 3, 2, *piece), BF),
        vm((3, 4, *piece), BF),
        vm((3, 3, *piece), BF),
        vm((4, 8, 768), F32),
        vm((8, 768), F32),
        vm((4, 3, 8, 768), F32),
        vm((2, 4, 64, 1024), F32),
        vm((2, 4, 64, 1024), F32),
        vm((2, 4, 64, 1024), BF),
        vm((2, 4, 64, 1024), BF),
        vm((2, 4, 64, 1024), BF),
        vm((2, 3, 64, 1024), BF),
        vm((2, 64, 1024), F32),
        vm((64, 1024), BF),
        vm((64, 1024), BF),
        pltpu.SemaphoreType.DMA((COPIES,)),
        pltpu.SemaphoreType.DMA((COPIES,)),
        pltpu.SemaphoreType.DMA((4,)),
    ]
    gw, gh, rb = pl.pallas_call(
        kernel,
        out_shape=(
            vm((1024, 5120), BF),
            vm((3, 16, 640), BF),
            vm((64, 1024), F32),
        ),
        in_specs=[anywhere, anywhere, in_vmem, in_vmem, in_vmem, in_vmem, anywhere],
        out_specs=(in_vmem,) * 3,
        scratch_shapes=scratch,
        compiler_params=pltpu.CompilerParams(
            collective_id=0, has_side_effects=True, vmem_limit_bytes=55 * 1000 * 1000
        ),
    )(
        hidden.reshape(3, 16, 5120),
        head_weight,
        target_ids,
        response_mask,
        advantages,
        seq_tokens,
        layer_grads.reshape(2, 4, 2, 64, 1024),
    )
    gh, gw, rb = pl.pallas_call(
        flush,
        out_shape=(
            jax.ShapeDtypeStruct((3, 16, 640), BF),
            jax.ShapeDtypeStruct((1024, 5120), BF),
            jax.ShapeDtypeStruct((64, 1024), F32),
        ),
        in_specs=[in_vmem] * 3,
        out_specs=(anywhere,) * 3,
        scratch_shapes=[pltpu.SemaphoreType.DMA((10,))],
        compiler_params=pltpu.CompilerParams(vmem_limit_bytes=16 * 1024 * 1024),
    )(gw, gh, rb)
    return gh.reshape(48, 640), gw, rb


def solution(mesh):
    split = Mesh(
        mesh.devices.reshape(2, 4, 2, 4, 2), ("dp_0", "dp_1", "dp_2", "vocab_0", "vocab_1")
    )
    return jax.shard_map(
        on_device,
        mesh=split,
        in_specs=(P(DP, None), P(DP_VOCAB, None), P(DP), P(DP), P(DP), P(DP), P(DP, None, VOCAB)),
        out_specs=(P(DP, VOCAB), P(DP_VOCAB, None), P(DP, VOCAB)),
        check_vma=False,
    )
```

```python
import functools

import jax
import jax.numpy as jnp
from jax import lax
from jax.experimental import pallas as pl
from jax.experimental.pallas import tpu as pltpu
from jax.sharding import Mesh
from jax.sharding import PartitionSpec as P

VOCAB = ("vocab_0", "vocab_1")
DP = ("dp_0", "dp_1", "dp_2")
DP_VOCAB = ("dp_0", "dp_1", "dp_2", "vocab_0", "vocab_1")
BF, F32 = jnp.bfloat16, jnp.float32

loss_scale = 16.0
entropy_coef = 0.1

COPIES = 160


def rem4(v):
    return lax.rem(v, 4)


class Net:
    def __init__(self, send_sems, recv_sems):
        self.send_sems, self.recv_sems, self.all = send_sems, recv_sems, []

    def copy(self, src, dst, dev):
        i = len(self.all)
        c = pltpu.make_async_remote_copy(
            src_ref=src,
            dst_ref=dst,
            send_sem=self.send_sems.at[i],
            recv_sem=self.recv_sems.at[i],
            device_id=dev,
            device_id_type=pl.DeviceIdType.MESH,
        )
        c.start()
        self.all.append(c)
        return c


class Ring4:
    def __init__(self, net, me, to, chunk, recv):
        self.net, self.me, self.to, self.chunk, self.recv = net, me, to, chunk, recv

    def far(self):
        t = rem4(self.me + 2)
        self.c1 = self.net.copy(self.chunk(t, 0), self.recv.at[0, 0], self.to(1))
        self.c2 = self.net.copy(self.chunk(t, 1), self.recv.at[1, 0], self.to(3))

    def near_plus(self):
        self.c3 = self.net.copy(self.chunk(rem4(self.me + 1), 1), self.recv.at[0, 1], self.to(1))

    def near_minus(self):
        self.c4 = self.net.copy(self.chunk(rem4(self.me + 3), 0), self.recv.at[1, 1], self.to(3))

    def near(self):
        self.near_plus()
        self.near_minus()

    def relay_plus(self):
        d = self.chunk(rem4(self.me + 1), 0)
        self.c1.wait_recv()
        d[...] = (d[...].astype(F32) + self.recv[0, 0].astype(F32)).astype(BF)
        self.c5 = self.net.copy(d, self.recv.at[0, 2], self.to(1))

    def relay_minus(self):
        d = self.chunk(rem4(self.me + 3), 1)
        self.c2.wait_recv()
        d[...] = (d[...].astype(F32) + self.recv[1, 0].astype(F32)).astype(BF)
        self.c6 = self.net.copy(d, self.recv.at[1, 2], self.to(3))

    def relay(self):
        self.relay_plus()
        self.relay_minus()

    def finish(self, put):
        for c in (self.c3, self.c4, self.c5, self.c6):
            c.wait_recv()
        r, mine = self.recv, self.chunk
        me = rem4(self.me)
        put(0, mine(me, 0)[...].astype(F32) + r[0, 2].astype(F32) + r[1, 1].astype(F32))
        put(1, mine(me, 1)[...].astype(F32) + r[0, 1].astype(F32) + r[1, 2].astype(F32))


def kernel(
    hid, w_hbm, tgt, msk, adv, seq, lg, w, gh, rb,
    g, h, logit, gt, own, snd, rcv, t_buf, r1, r1y, r1z, u0, u1, u2, r2, v, r3,
    st_s, st_c, st_r, b_sib, b_own, b_s, b_r, b, b_rz, b_u, b_y, b_ry,
    send_sems, recv_sems, local_sems,
):
    yh, z, c = lax.axis_index("dp_0"), lax.axis_index("dp_1"), lax.axis_index("dp_2")
    x, yl = lax.axis_index("vocab_0"), lax.axis_index("vocab_1")
    y = 2 * yh + yl
    k = lax.rem(x + yh + yl, 2)

    def to_x(d):
        return {"vocab_0": rem4(x + d)}

    def to_z(d):
        return {"dp_1": rem4(z + d)}

    def to_y(d):
        n = rem4(y + d)
        return {"dp_0": n // 2, "vocab_1": lax.rem(n, 2)}

    y_other = {"dp_0": 1 - yh, "vocab_1": 1 - yl}
    y_same = {"vocab_1": 1 - yl}
    core = {"dp_2": 1 - c}

    net = Net(send_sems, recv_sems)

    ld_h = pltpu.make_async_copy(hid, h.at[:, c, yh, z], local_sems.at[0])
    ld_h.start()
    ld_bs = pltpu.make_async_copy(lg.at[:, :, 1 - c], b_sib, local_sems.at[1])
    ld_bs.start()
    ld_w = pltpu.make_async_copy(w_hbm, w, local_sems.at[2])
    ld_w.start()
    ld_bo = pltpu.make_async_copy(lg.at[:, :, c], b_own, local_sems.at[3])
    ld_bo.start()

    barrier = pltpu.get_barrier_semaphore()
    peers = [core] + [f(d) for f in (to_x, to_y, to_z) for d in (1, 3)]
    for p in peers:
        pl.semaphore_signal(barrier, inc=1, device_id=p, device_id_type=pl.DeviceIdType.MESH)
    pl.semaphore_wait(barrier, len(peers))
    ld_h.wait()

    mine = pl.ds(pl.multiple_of(k * 2560, 128), 2560)
    other = pl.ds(pl.multiple_of((1 - k) * 2560, 128), 2560)
    lower = pl.ds(pl.multiple_of(k * 2560, 128), 1280)
    upper = pl.ds(pl.multiple_of(k * 2560 + 1280, 128), 1280)

    def piece(j, hi, zz, cols):
        return h.at[j, c, hi, zz, :, cols]

    def hop(j, hi, zz, cols, dev):
        ref = piece(j, hi, zz, cols)
        return net.copy(ref, ref, dev)

    yo, zm, zp, z2 = 1 - yh, rem4(z + 3), rem4(z + 1), rem4(z + 2)
    sides = (to_x(1), to_x(3), y_same)
    ag = [{} for _ in range(3)]
    for j in range(3):
        ag[j]["zm"] = hop(j, yh, z, mine, to_z(1))
        ag[j]["zp"] = hop(j, yh, z, mine, to_z(3))
        ag[j]["yo"] = hop(j, yh, z, mine, y_other)

    def across(j, p, hi, zz):
        ag[j]["b%d" % p] = hop(j, hi, zz, mine, sides[(p + j) % 3])

    def relay_near(j):
        a = ag[j]
        a["zm"].wait_recv()
        a["z2l"] = hop(j, yh, zm, lower, to_z(1))
        across(j, 0, yh, zm)
        a["zp"].wait_recv()
        a["z2u"] = hop(j, yh, zp, upper, to_z(3))
        across(j, 1, yh, zp)

    def relay_other(j):
        a = ag[j]
        a["yo"].wait_recv()
        a["zmo"] = hop(j, yo, z, mine, to_z(1))
        a["zpo"] = hop(j, yo, z, mine, to_z(3))
        across(j, 2, yo, z)

    def relay_far(j):
        a = ag[j]
        a["z2l"].wait_recv()
        a["z2u"].wait_recv()
        a["yo2"] = hop(j, yh, z2, mine, y_other)
        across(j, 5, yh, z2)

    def relay_last(j):
        a = ag[j]
        a["zmo"].wait_recv()
        across(j, 3, yo, zm)
        a["zpo"].wait_recv()
        across(j, 4, yo, zp)

    def relay_end(j):
        a = ag[j]
        a["yo2"].wait_recv()
        across(j, 6, yo, z2)
        ref = h.at[j, c, :, :, :, mine]
        a["d0"] = net.copy(ref, ref, core)

    def gather_across(j):
        for p in range(7):
            ag[j]["b%d" % p].wait_recv()
        ref = h.at[j, c, :, :, :, other]
        ag[j]["d1"] = net.copy(ref, ref, core)

    def gather_done(j):
        ag[j]["d0"].wait_recv()
        ag[j]["d1"].wait_recv()

    def bucket_pair():
        ld_bs.wait()
        b_s[...] = b_sib[...].astype(BF)
        return net.copy(b_s, b_r, core)

    def bucket_sum(cp):
        ld_bo.wait()
        cp.wait_recv()
        b[...] = (b_own[...] + b_r[...].astype(F32)).astype(BF)

    bz = Ring4(net, z, to_z, lambda t, hf: b.at[hf, t], b_rz)

    def b_put(hf, val):
        b_u[hf] = val

    def logits(j, cols, first):
        def block(i, _):
            rows = pl.ds(pl.multiple_of(i * 512, 512), 512)
            part = lax.dot_general(
                w[rows, cols], h[j, :, :, :, :, cols].reshape(256, 2560),
                (((1,), (1,)), ((), ())), preferred_element_type=F32,
            )
            if not first:
                part = part + logit[rows, j * 256 : (j + 1) * 256]
            logit[rows, j * 256 : (j + 1) * 256] = part
            return 0

        lax.fori_loop(0, 2, block, 0)

    def place_meta():
        r8 = lax.broadcasted_iota(jnp.int32, (8, 48), 0)
        rows = jnp.zeros((8, 48), F32)
        for r, ref in enumerate((tgt, msk, adv)):
            rows = jnp.where(r8 == r, ref[...].astype(F32).reshape(1, 48), rows)
        count = jnp.sum(seq[...].astype(F32).reshape(1, 8), axis=1, keepdims=True)
        token = lax.broadcasted_iota(jnp.int32, (48, 256), 0)
        lane = lax.broadcasted_iota(jnp.int32, (48, 256), 1)
        base = (c * 8 + yh * 4 + z) * 16
        for j in range(3):
            hot = jnp.where(lane - base == token - 16 * j, 1.0, 0.0)
            hot = jnp.where((token >= 16 * j) & (token < 16 * j + 16), hot, 0.0)
            put = lax.dot_general(
                rows, hot, (((1,), (0,)), ((), ())),
                preferred_element_type=F32, precision=lax.Precision.HIGHEST,
            )
            r_id = lax.broadcasted_iota(jnp.int32, (8, 256), 0)
            tile = jnp.where(r_id == 6, count, 0.0)
            for r in range(3):
                tile = jnp.where(r_id == 3 + r, put[r : r + 1], tile)
            st_c[:, j * 256 : (j + 1) * 256] = tile

    row_id = lax.broadcasted_iota(jnp.int32, (8, 768), 0)

    def local_stats():
        def top(i, m):
            blk = logit[pl.ds(pl.multiple_of(i * 64, 64), 64)]
            return jnp.maximum(m, jnp.max(blk.reshape(8, 8, 768), axis=0))

        m8 = lax.fori_loop(0, 16, top, jnp.full((8, 768), -jnp.inf, F32))
        m = jnp.max(m8, axis=0, keepdims=True)

        def sums(i, se):
            blk = logit[pl.ds(pl.multiple_of(i * 64, 64), 64)]
            e = jnp.exp(blk - m)
            return (
                se[0] + jnp.sum(e.reshape(8, 8, 768), axis=0),
                se[1] + jnp.sum((e * blk).reshape(8, 8, 768), axis=0),
            )

        zero = jnp.zeros((8, 768), F32)
        s8, e8 = lax.fori_loop(0, 16, sums, (zero, zero))
        s = jnp.sum(s8, axis=0, keepdims=True)
        e = jnp.sum(e8, axis=0, keepdims=True)
        tile = st_c[...]
        tile = jnp.where(row_id == 0, m, tile)
        tile = jnp.where(row_id == 1, s, tile)
        tile = jnp.where(row_id == 2, e, tile)
        return tile

    phases = (
        [core] + [to_x(d) for d in (1, 2, 3)] + [{**core, **to_x(d)} for d in (1, 2, 3)],
        [to_y(d) for d in (1, 2, 3)],
        [to_z(d) for d in (1, 2, 3)],
    )
    st = {}

    def stats_send(ph, tile):
        st_s[ph] = tile
        st[ph] = [net.copy(st_s.at[ph], st_r.at[ph, d], dev) for d, dev in enumerate(phases[ph])]

    def stats_recv(ph):
        tiles = [st_s[ph]]
        for d, cp in enumerate(st[ph]):
            cp.wait_recv()
            tiles.append(st_r[ph, d])
        m = functools.reduce(jnp.maximum, [t[0:1] for t in tiles])
        total = None
        for t in tiles:
            f = jnp.exp(t[0:1] - m)
            scaled = t * jnp.where((row_id == 1) | (row_id == 2), f, 1.0)
            total = scaled if total is None else total + scaled
        return jnp.where(row_id == 0, m, total)

    def stats_next(ph):
        stats_send(ph, stats_recv(ph - 1))

    def stats_end():
        st_c[...] = stats_recv(2)

    def factor_of(count_row):
        return (loss_scale * 768.0) / (count_row / 8.0)

    first_id = ((yh * 8 + z * 2 + c) * 8 + x * 2 + yl) * 1024

    def grads():
        tile = st_c[...]
        m, s, e = tile[0:1], tile[1:2], tile[2:3]
        target = tile[3:4] / 8.0
        mask = tile[4:5] / 8.0
        adv = tile[5:6] / 8.0
        inv = 1.0 / s
        mean = e * inv
        wt = factor_of(tile[6:7]) * mask
        wa = wt * adv
        wb = wt * entropy_coef

        def block(i, _):
            rows = pl.ds(pl.multiple_of(i * 128, 128), 128)
            l = logit[rows]
            ids = (first_id + i * 128 + lax.broadcasted_iota(jnp.int32, (128, 768), 0)).astype(F32)
            p = jnp.exp(l - m) * inv
            val = p * (wa + wb * (l - mean))
            val = jnp.where(ids == target, val - wa, val)
            g[rows] = val.astype(BF)
            for j in range(3):
                for cc in range(2):
                    at = (2 * j + cc) * 128
                    gt[(c if cc == 0 else 1 - c), j, :, rows] = val[:, at : at + 128].T.astype(BF)
            return 0

        lax.fori_loop(0, 8, block, 0)

    xs_of = [rem4(x + 2), rem4(x + 1), rem4(x + 3), x]
    pair = {}

    def terms(s, side):
        cols = pl.ds(pl.multiple_of(xs_of[s] * 1280, 128), 1280)
        acc = jnp.dot(gt[side].reshape(384, 1024), w[:, cols], preferred_element_type=F32)
        for lo in range(2):
            part = acc[:, lo * 640 : (lo + 1) * 640].reshape(3, 2, 4, 16, 640).astype(BF)
            if side == 0:
                own[s % 2, lo] = part
            else:
                snd[s, lo] = part
        if side == 1:
            pair[s] = net.copy(snd.at[s], rcv.at[s], core)

    def joined(s):
        pair[s].wait_recv()
        for lo in range(2):
            t_buf[:, :, :, xs_of[s], lo] = (
                own[s % 2, lo].astype(F32) + rcv[s, lo].astype(F32)
            ).astype(BF)

    t0, t1, t2 = t_buf.at[0], t_buf.at[1], t_buf.at[2]
    ring_x = Ring4(net, x, to_x, lambda t, hf: t0.at[hf, :, t], r1)
    ring_y, ring_z = [], []
    for s in range(4):
        ring_y.append(
            Ring4(
                net, y, to_y,
                lambda t, hf, s=s: t1.at[t // 2, 2 * hf : 2 * hf + 2, xs_of[s], lax.rem(t, 2)],
                r1y.at[s],
            )
        )
        ring_z.append(Ring4(net, z, to_z, lambda t, hf, s=s: t2.at[hf, t, xs_of[s]], r1z.at[s]))

    def put_x(hf, val):
        u0[hf] = val.astype(BF)

    def put_y(s):
        def put(hf, val):
            u1[2 * hf : 2 * hf + 2, xs_of[s]] = val.astype(BF)

        return put

    def put_z(s):
        def put(hf, val):
            u2[hf, xs_of[s]] = val.astype(BF)

        return put

    def start(s):
        for r in (ring_y[s], ring_z[s]):
            r.far()
            r.near()

    def relay(s):
        ring_y[s].relay()
        ring_z[s].relay()

    def finish(s):
        ring_y[s].finish(put_y(s))
        ring_z[s].finish(put_z(s))

    def begin_second(j):
        second[j].far()
        second[j].near()

    second = [
        Ring4(
            net, y, to_y,
            lambda t, hf: u0.at[t // 2, 2 * hf : 2 * hf + 2, lax.rem(t, 2)], r2.at[0],
        ),
        Ring4(net, z, to_z, lambda t, hf: u1.at[t, 2 * hf : 2 * hf + 2], r2.at[1]),
        Ring4(net, x, to_x, lambda t, hf: u2.at[hf, t], r2.at[2]),
    ]

    def put2(j):
        def put(hf, val):
            v[j, 2 * hf : 2 * hf + 2] = val.astype(BF)

        return put

    last_axis = [(z, to_z), (x, to_x), (y, to_y)]
    last = [None] * 3

    def third(j):
        me, to = last_axis[j]
        last[j] = [net.copy(v.at[j, rem4(me + d)], r3.at[j, d - 1], to(d)) for d in (1, 2, 3)]

    def rs_end(j):
        total = v[j, last_axis[j][0]].astype(F32)
        for d in range(3):
            last[j][d].wait_recv()
            total = total + r3[j, d].astype(F32)
        gh[j] = total.astype(BF)

    def end_second(j):
        second[j].finish(put2(j))
        third(j)

    def weight_grad(n):
        cols = slice(n * 512, (n + 1) * 512)
        hn = h[:, :, :, :, :, cols].reshape(768, 512)
        w[:, cols] = jnp.dot(g[...], hn, preferred_element_type=F32).astype(BF)

    bp = bucket_pair()
    place_meta()
    relay_near(0)
    relay_near(1)
    relay_other(0)
    relay_near(2)
    relay_other(1)
    relay_other(2)
    relay_far(0)
    relay_far(1)
    relay_last(0)
    relay_far(2)
    relay_end(0)
    relay_last(1)
    relay_end(1)
    ld_w.wait()
    ag[0]["d0"].wait_recv()
    logits(0, mine, True)
    relay_last(2)
    relay_end(2)
    bucket_sum(bp)
    bz.far()
    bz.near()
    ag[1]["d0"].wait_recv()
    logits(1, mine, True)
    gather_across(0)
    gather_across(1)
    ag[2]["d0"].wait_recv()
    logits(2, mine, True)
    ag[0]["d1"].wait_recv()
    logits(0, other, False)
    gather_across(2)
    bz.relay()
    ag[1]["d1"].wait_recv()
    logits(1, other, False)
    ag[2]["d1"].wait_recv()
    logits(2, other, False)
    stats_send(0, local_stats())
    bz.finish(b_put)
    b_y[...] = b_u[1 - yh].astype(BF)
    stats_next(1)
    stats_next(2)
    stats_end()
    by = net.copy(b_y, b_ry, {"dp_0": 1 - yh})
    grads()
    terms(0, 1)
    terms(0, 0)
    terms(1, 1)
    joined(0)
    ring_x.far()
    start(0)
    terms(1, 0)
    terms(2, 1)
    joined(1)
    ring_x.near_plus()
    start(1)
    terms(2, 0)
    terms(3, 1)
    relay(0)
    joined(2)
    ring_x.near_minus()
    start(2)
    terms(3, 0)
    ring_x.relay_plus()
    ring_x.relay_minus()
    relay(1)
    joined(3)
    start(3)
    weight_grad(0)
    weight_grad(1)
    relay(2)
    finish(0)
    weight_grad(2)
    finish(1)
    relay(3)
    weight_grad(3)
    weight_grad(4)
    finish(2)
    ring_x.finish(put_x)
    begin_second(0)
    finish(3)
    begin_second(1)
    begin_second(2)
    by.wait_recv()
    rb[...] = (b_u[yh] + b_ry[...].astype(F32)) * factor_of(st_c[6:7, 0:1])
    weight_grad(5)
    weight_grad(6)
    second[0].relay()
    weight_grad(7)
    second[1].relay()
    second[2].relay()
    weight_grad(8)
    end_second(0)
    weight_grad(9)
    end_second(1)
    end_second(2)
    rs_end(0)
    rs_end(1)
    rs_end(2)
    for cp in net.all:
        cp.wait_send()


def flush(gw_in, gh_in, rb_in, gh, gw, rb, sems):
    copies = [
        pltpu.make_async_copy(gw_in.at[rows], gw.at[rows], sems.at[i])
        for i, rows in enumerate(pl.ds(128 * k, 128) for k in range(8))
    ]
    copies.append(pltpu.make_async_copy(gh_in, gh, sems.at[8]))
    copies.append(pltpu.make_async_copy(rb_in, rb, sems.at[9]))
    for cp in copies:
        cp.start()
    for cp in copies:
        cp.wait()


def on_device(hidden, head_weight, target_ids, response_mask, advantages, seq_tokens, layer_grads):
    vm = pltpu.VMEM
    anywhere = pl.BlockSpec(memory_space=pl.ANY)
    in_vmem = pl.BlockSpec(memory_space=pltpu.VMEM)
    piece = (16, 640)
    scratch = [
        vm((1024, 768), BF),
        vm((3, 2, 2, 4, 16, 5120), BF),
        vm((1024, 768), F32),
        vm((2, 3, 128, 1024), BF),
        vm((2, 2, 3, 2, 4, *piece), BF),
        vm((4, 2, 3, 2, 4, *piece), BF),
        vm((4, 2, 3, 2, 4, *piece), BF),
        vm((3, 2, 4, 4, 2, *piece), BF),
        vm((2, 3, 4, 2, *piece), BF),
        vm((4, 2, 3, 2, *piece), BF),
        vm((4, 2, 3, 2, *piece), BF),
        vm((2, 4, 2, *piece), BF),
        vm((4, 4, *piece), BF),
        vm((2, 4, 2, *piece), BF),
        vm((3, 2, 3, 2, *piece), BF),
        vm((3, 4, *piece), BF),
        vm((3, 3, *piece), BF),
        vm((3, 8, 768), F32),
        vm((8, 768), F32),
        vm((3, 7, 8, 768), F32),
        vm((2, 4, 64, 1024), F32),
        vm((2, 4, 64, 1024), F32),
        vm((2, 4, 64, 1024), BF),
        vm((2, 4, 64, 1024), BF),
        vm((2, 4, 64, 1024), BF),
        vm((2, 3, 64, 1024), BF),
        vm((2, 64, 1024), F32),
        vm((64, 1024), BF),
        vm((64, 1024), BF),
        pltpu.SemaphoreType.DMA((COPIES,)),
        pltpu.SemaphoreType.DMA((COPIES,)),
        pltpu.SemaphoreType.DMA((4,)),
    ]
    gw, gh, rb = pl.pallas_call(
        kernel,
        out_shape=(
            vm((1024, 5120), BF),
            vm((3, 16, 640), BF),
            vm((64, 1024), F32),
        ),
        in_specs=[anywhere, anywhere, in_vmem, in_vmem, in_vmem, in_vmem, anywhere],
        out_specs=(in_vmem,) * 3,
        scratch_shapes=scratch,
        compiler_params=pltpu.CompilerParams(
            collective_id=0, has_side_effects=True, vmem_limit_bytes=55 * 1000 * 1000
        ),
    )(
        hidden.reshape(3, 16, 5120),
        head_weight,
        target_ids,
        response_mask,
        advantages,
        seq_tokens,
        layer_grads.reshape(2, 4, 2, 64, 1024),
    )
    gh, gw, rb = pl.pallas_call(
        flush,
        out_shape=(
            jax.ShapeDtypeStruct((3, 16, 640), BF),
            jax.ShapeDtypeStruct((1024, 5120), BF),
            jax.ShapeDtypeStruct((64, 1024), F32),
        ),
        in_specs=[in_vmem] * 3,
        out_specs=(anywhere,) * 3,
        scratch_shapes=[pltpu.SemaphoreType.DMA((10,))],
        compiler_params=pltpu.CompilerParams(vmem_limit_bytes=16 * 1024 * 1024),
    )(gw, gh, rb)
    return gh.reshape(48, 640), gw, rb


def solution(mesh):
    split = Mesh(
        mesh.devices.reshape(2, 4, 2, 4, 2), ("dp_0", "dp_1", "dp_2", "vocab_0", "vocab_1")
    )
    return jax.shard_map(
        on_device,
        mesh=split,
        in_specs=(P(DP, None), P(DP_VOCAB, None), P(DP), P(DP), P(DP), P(DP), P(DP, None, VOCAB)),
        out_specs=(P(DP, VOCAB), P(DP_VOCAB, None), P(DP, VOCAB)),
        check_vma=False,
    )
```

```python
import functools

import jax
import jax.numpy as jnp
from jax import lax
from jax.experimental import pallas as pl
from jax.experimental.pallas import tpu as pltpu
from jax.sharding import Mesh
from jax.sharding import PartitionSpec as P

VOCAB = ("vocab_0", "vocab_1")
DP = ("dp_0", "dp_1", "dp_2")
DP_VOCAB = ("dp_0", "dp_1", "dp_2", "vocab_0", "vocab_1")
BF, F32 = jnp.bfloat16, jnp.float32

loss_scale = 16.0
entropy_coef = 0.1

COPIES = 168


def rem4(v):
    return lax.rem(v, 4)


class Net:
    def __init__(self, send_sems, recv_sems):
        self.send_sems, self.recv_sems, self.all = send_sems, recv_sems, []

    def copy(self, src, dst, dev):
        i = len(self.all)
        c = pltpu.make_async_remote_copy(
            src_ref=src,
            dst_ref=dst,
            send_sem=self.send_sems.at[i],
            recv_sem=self.recv_sems.at[i],
            device_id=dev,
            device_id_type=pl.DeviceIdType.MESH,
        )
        c.start()
        self.all.append(c)
        return c


class Ring4:
    def __init__(self, net, me, to, chunk, recv):
        self.net, self.me, self.to, self.chunk, self.recv = net, me, to, chunk, recv

    def far(self):
        t = rem4(self.me + 2)
        self.c1 = self.net.copy(self.chunk(t, 0), self.recv.at[0, 0], self.to(1))
        self.c2 = self.net.copy(self.chunk(t, 1), self.recv.at[1, 0], self.to(3))

    def near_plus(self):
        self.c3 = self.net.copy(self.chunk(rem4(self.me + 1), 1), self.recv.at[0, 1], self.to(1))

    def near_minus(self):
        self.c4 = self.net.copy(self.chunk(rem4(self.me + 3), 0), self.recv.at[1, 1], self.to(3))

    def near(self):
        self.near_plus()
        self.near_minus()

    def relay_plus(self):
        d = self.chunk(rem4(self.me + 1), 0)
        self.c1.wait_recv()
        d[...] = (d[...].astype(F32) + self.recv[0, 0].astype(F32)).astype(BF)
        self.c5 = self.net.copy(d, self.recv.at[0, 2], self.to(1))

    def relay_minus(self):
        d = self.chunk(rem4(self.me + 3), 1)
        self.c2.wait_recv()
        d[...] = (d[...].astype(F32) + self.recv[1, 0].astype(F32)).astype(BF)
        self.c6 = self.net.copy(d, self.recv.at[1, 2], self.to(3))

    def relay(self):
        self.relay_plus()
        self.relay_minus()

    def finish(self, put):
        for c in (self.c3, self.c4, self.c5, self.c6):
            c.wait_recv()
        r, mine = self.recv, self.chunk
        me = rem4(self.me)
        put(0, mine(me, 0)[...].astype(F32) + r[0, 2].astype(F32) + r[1, 1].astype(F32))
        put(1, mine(me, 1)[...].astype(F32) + r[0, 1].astype(F32) + r[1, 2].astype(F32))


def kernel(
    hid, w_hbm, tgt, msk, adv, seq, lg, w, gh, rb,
    g, h, logit, gt, half, rcv, t_buf, r1, r1y, r1z, u0, u1, u2, r2, v, r3,
    st_s, st_c, st_r, put_at, mt_s, mt_c, mt_r, b_sib, b_own, b_s, b_r, b, b_rz, b_u, b_y, b_ry,
    send_sems, recv_sems, local_sems,
):
    yh, z, c = lax.axis_index("dp_0"), lax.axis_index("dp_1"), lax.axis_index("dp_2")
    x, yl = lax.axis_index("vocab_0"), lax.axis_index("vocab_1")
    y = 2 * yh + yl
    k = lax.rem(x + yh + yl, 2)

    def to_x(d):
        return {"vocab_0": rem4(x + d)}

    def to_z(d):
        return {"dp_1": rem4(z + d)}

    def to_y(d):
        n = rem4(y + d)
        return {"dp_0": n // 2, "vocab_1": lax.rem(n, 2)}

    y_other = {"dp_0": 1 - yh, "vocab_1": 1 - yl}
    y_same = {"vocab_1": 1 - yl}
    core = {"dp_2": 1 - c}

    net = Net(send_sems, recv_sems)

    ld_h = pltpu.make_async_copy(hid, h.at[:, c, yh, z], local_sems.at[0])
    ld_h.start()
    ld_bs = pltpu.make_async_copy(lg.at[:, :, 1 - c], b_sib, local_sems.at[1])
    ld_bs.start()
    ld_w = pltpu.make_async_copy(w_hbm, w, local_sems.at[2])
    ld_w.start()
    ld_bo = pltpu.make_async_copy(lg.at[:, :, c], b_own, local_sems.at[3])
    ld_bo.start()

    barrier = pltpu.get_barrier_semaphore()
    peers = [core] + [f(d) for f in (to_x, to_y, to_z) for d in (1, 3)]
    for p in peers:
        pl.semaphore_signal(barrier, inc=1, device_id=p, device_id_type=pl.DeviceIdType.MESH)
    pl.semaphore_wait(barrier, len(peers))
    ld_h.wait()

    mine = pl.ds(pl.multiple_of(k * 2560, 128), 2560)
    other = pl.ds(pl.multiple_of((1 - k) * 2560, 128), 2560)
    lower = pl.ds(pl.multiple_of(k * 2560, 128), 1280)
    upper = pl.ds(pl.multiple_of(k * 2560 + 1280, 128), 1280)

    def piece(j, hi, zz, cols):
        return h.at[j, c, hi, zz, :, cols]

    def hop(j, hi, zz, cols, dev):
        ref = piece(j, hi, zz, cols)
        return net.copy(ref, ref, dev)

    yo, zm, zp, z2 = 1 - yh, rem4(z + 3), rem4(z + 1), rem4(z + 2)
    sides = (to_x(1), to_x(3), y_same)
    ag = [{} for _ in range(3)]
    for j in range(3):
        ag[j]["zm"] = hop(j, yh, z, mine, to_z(1))
        ag[j]["zp"] = hop(j, yh, z, mine, to_z(3))
        ag[j]["yo"] = hop(j, yh, z, mine, y_other)

    def across(j, p, hi, zz):
        ag[j]["b%d" % p] = hop(j, hi, zz, mine, sides[(p + j) % 3])

    def relay_near(j):
        a = ag[j]
        a["zm"].wait_recv()
        a["z2l"] = hop(j, yh, zm, lower, to_z(1))
        across(j, 0, yh, zm)
        a["zp"].wait_recv()
        a["z2u"] = hop(j, yh, zp, upper, to_z(3))
        across(j, 1, yh, zp)

    def relay_other(j):
        a = ag[j]
        a["yo"].wait_recv()
        a["zmo"] = hop(j, yo, z, mine, to_z(1))
        a["zpo"] = hop(j, yo, z, mine, to_z(3))
        across(j, 2, yo, z)

    def relay_far(j):
        a = ag[j]
        a["z2l"].wait_recv()
        a["z2u"].wait_recv()
        a["yo2"] = hop(j, yh, z2, mine, y_other)
        across(j, 5, yh, z2)

    def relay_last(j):
        a = ag[j]
        a["zmo"].wait_recv()
        across(j, 3, yo, zm)
        a["zpo"].wait_recv()
        across(j, 4, yo, zp)

    def relay_end(j):
        a = ag[j]
        a["yo2"].wait_recv()
        across(j, 6, yo, z2)
        ref = h.at[j, c, :, :, :, mine]
        a["d0"] = net.copy(ref, ref, core)

    def gather_across(j):
        for p in range(7):
            ag[j]["b%d" % p].wait_recv()
        ref = h.at[j, c, :, :, :, other]
        ag[j]["d1"] = net.copy(ref, ref, core)

    def gather_done(j):
        ag[j]["d0"].wait_recv()
        ag[j]["d1"].wait_recv()

    def bucket_pair():
        ld_bs.wait()
        b_s[...] = b_sib[...].astype(BF)
        return net.copy(b_s, b_r, core)

    def bucket_sum(cp):
        ld_bo.wait()
        cp.wait_recv()
        b[...] = (b_own[...] + b_r[...].astype(F32)).astype(BF)

    bz = Ring4(net, z, to_z, lambda t, hf: b.at[hf, t], b_rz)

    def b_put(hf, val):
        b_u[hf] = val

    def logits(j, cols, first):
        def block(i, _):
            rows = pl.ds(pl.multiple_of(i * 512, 512), 512)
            part = lax.dot_general(
                w[rows, cols], h[j, :, :, :, :, cols].reshape(256, 2560),
                (((1,), (1,)), ((), ())), preferred_element_type=F32,
            )
            if not first:
                part = part + logit[rows, j * 256 : (j + 1) * 256]
            logit[rows, j * 256 : (j + 1) * 256] = part
            return 0

        lax.fori_loop(0, 2, block, 0)

    def place_meta():
        r8 = lax.broadcasted_iota(jnp.int32, (8, 48), 0)
        rows = jnp.zeros((8, 48), F32)
        for r, ref in enumerate((tgt, msk, adv)):
            rows = jnp.where(r8 == r, ref[...].astype(F32).reshape(1, 48), rows)
        count = jnp.sum(seq[...].astype(F32).reshape(1, 8), axis=1, keepdims=True)
        token = lax.broadcasted_iota(jnp.int32, (48, 256), 0)
        lane = lax.broadcasted_iota(jnp.int32, (48, 256), 1)
        base = (c * 8 + yh * 4 + z) * 16
        for j in range(3):
            hot = jnp.where(lane - base == token - 16 * j, 1.0, 0.0)
            hot = jnp.where((token >= 16 * j) & (token < 16 * j + 16), hot, 0.0)
            put = lax.dot_general(
                rows, hot, (((1,), (0,)), ((), ())),
                preferred_element_type=F32, precision=lax.Precision.HIGHEST,
            )
            r_id = lax.broadcasted_iota(jnp.int32, (8, 256), 0)
            tile = jnp.where(r_id == 6, count, 0.0)
            for r in range(3):
                tile = jnp.where(r_id == 3 + r, put[r : r + 1], tile)
            put_at[:, j * 256 : (j + 1) * 256] = tile

        pack(mt_s.at[0], [put_at[r : r + 1] for r in (3, 4, 5)])
        mt_s[0, 6:8] = jnp.broadcast_to(count, (2, 384))
        meta_send(0)

    def pack(ref, rows):
        for i, row in enumerate(rows):
            ref[2 * i : 2 * i + 1] = row[:, :384]
            ref[2 * i + 1 : 2 * i + 2] = row[:, 384:]

    def unpack(tile, i):
        return jnp.concatenate([tile[2 * i : 2 * i + 1], tile[2 * i + 1 : 2 * i + 2]], axis=1)

    meta_phases = ([core], [to_y(d) for d in (1, 2, 3)], [to_z(d) for d in (1, 2, 3)])
    mt = {}

    def meta_send(ph):
        mt[ph] = [
            net.copy(mt_s.at[ph], mt_r.at[ph, d], dev) for d, dev in enumerate(meta_phases[ph])
        ]

    def meta_sum(ph):
        total = mt_s[ph]
        for d, cp in enumerate(mt[ph]):
            cp.wait_recv()
            total = total + mt_r[ph, d]
        return total

    def meta_next(ph):
        mt_s[ph] = meta_sum(ph - 1)
        meta_send(ph)

    def local_stats():
        def top(i, m):
            blk = logit[pl.ds(pl.multiple_of(i * 64, 64), 64)]
            return jnp.maximum(m, jnp.max(blk.reshape(8, 8, 768), axis=0))

        m8 = lax.fori_loop(0, 16, top, jnp.full((8, 768), -jnp.inf, F32))
        m = jnp.max(m8, axis=0, keepdims=True)

        def sums(i, se):
            blk = logit[pl.ds(pl.multiple_of(i * 64, 64), 64)]
            e = jnp.exp(blk - m)
            return (
                se[0] + jnp.sum(e.reshape(8, 8, 768), axis=0),
                se[1] + jnp.sum((e * blk).reshape(8, 8, 768), axis=0),
            )

        zero = jnp.zeros((8, 768), F32)
        s8, e8 = lax.fori_loop(0, 16, sums, (zero, zero))
        s = jnp.sum(s8, axis=0, keepdims=True)
        e = jnp.sum(e8, axis=0, keepdims=True)
        pack(st_s.at[0], (m, s, e))
        st_s[0, 6:8] = jnp.zeros((2, 384), F32)

    phases = (
        [core] + [to_x(d) for d in (1, 2, 3)] + [{**core, **to_x(d)} for d in (1, 2, 3)],
        [to_y(d) for d in (1, 2, 3)],
        [to_z(d) for d in (1, 2, 3)],
    )
    st = {}

    def stats_send(ph):
        st[ph] = [net.copy(st_s.at[ph], st_r.at[ph, d], dev) for d, dev in enumerate(phases[ph])]

    def stats_sum(ph, out):
        tiles = [st_s[ph]]
        for d, cp in enumerate(st[ph]):
            cp.wait_recv()
            tiles.append(st_r[ph, d])
        m = functools.reduce(jnp.maximum, [t[0:2] for t in tiles])
        scales = [jnp.exp(t[0:2] - m) for t in tiles]
        out[0:2] = m
        for at in (2, 4):
            out[at : at + 2] = sum(t[at : at + 2] * f for t, f in zip(tiles, scales))
        out[6:8] = jnp.zeros((2, 384), F32)

    def stats_next(ph):
        stats_sum(ph - 1, st_s.at[ph])
        stats_send(ph)

    def stats_end():
        stats_sum(2, st_c)
        mt_c[...] = meta_sum(2)

    def factor_of(count_row):
        return (loss_scale * 768.0) / (count_row / 2.0)

    first_id = ((yh * 8 + z * 2 + c) * 8 + x * 2 + yl) * 1024

    def grads():
        tile = st_c[...]
        m, s, e = (unpack(tile, i) for i in range(3))
        target, mask, adv = (unpack(mt_c[...], i) / 2.0 for i in range(3))
        inv = 1.0 / s
        mean = e * inv
        wt = factor_of(mt_c[6:7, 0:1]) * mask
        wa = wt * adv
        wb = wt * entropy_coef

        def block(i, _):
            rows = pl.ds(pl.multiple_of(i * 128, 128), 128)
            l = logit[rows]
            ids = (first_id + i * 128 + lax.broadcasted_iota(jnp.int32, (128, 768), 0)).astype(F32)
            p = jnp.exp(l - m) * inv
            val = p * (wa + wb * (l - mean))
            val = jnp.where(ids == target, val - wa, val)
            g[rows] = val.astype(BF)
            for j in range(3):
                for cc in range(2):
                    at = (2 * j + cc) * 128
                    gt[(c if cc == 0 else 1 - c), j, :, rows] = val[:, at : at + 128].T.astype(BF)
            return 0

        lax.fori_loop(0, 8, block, 0)

    xs_of = [rem4(x + 2), rem4(x + 1), rem4(x + 3), x]
    pair = {}

    def product(side, block, slot):
        cols = pl.ds(pl.multiple_of(block * 1280, 128), 1280)
        acc = jnp.dot(gt[side].reshape(384, 1024), w[:, cols], preferred_element_type=F32)
        for lo in range(2):
            part = acc[:, lo * 640 : (lo + 1) * 640]
            half[slot, lo] = part.reshape(3, 2, 4, 16, 640).astype(BF)

    def cross(s):
        pair[s] = net.copy(half.at[2 + s], rcv.at[s], core)

    def terms(s):
        def side(i, _):
            block = xs_of[s] + i * (xs_of[s + 1] - xs_of[s])
            product(i, block, s % 2 + i * (3 + s - s % 2))
            return 0

        lax.fori_loop(0, 2, side, 0)
        cross(s + 1)

    def joined(s):
        pair[s].wait_recv()
        for lo in range(2):
            t_buf[:, :, :, xs_of[s], lo] = (
                half[s % 2, lo].astype(F32) + rcv[s, lo].astype(F32)
            ).astype(BF)

    t0, t1, t2 = t_buf.at[0], t_buf.at[1], t_buf.at[2]
    ring_x = Ring4(net, x, to_x, lambda t, hf: t0.at[hf, :, t], r1)
    ring_y, ring_z = [], []
    for s in range(4):
        ring_y.append(
            Ring4(
                net, y, to_y,
                lambda t, hf, s=s: t1.at[t // 2, 2 * hf : 2 * hf + 2, xs_of[s], lax.rem(t, 2)],
                r1y.at[s],
            )
        )
        ring_z.append(Ring4(net, z, to_z, lambda t, hf, s=s: t2.at[hf, t, xs_of[s]], r1z.at[s]))

    def put_x(hf, val):
        u0[hf] = val.astype(BF)

    def put_y(s):
        def put(hf, val):
            u1[2 * hf : 2 * hf + 2, xs_of[s]] = val.astype(BF)

        return put

    def put_z(s):
        def put(hf, val):
            u2[hf, xs_of[s]] = val.astype(BF)

        return put

    def start(s):
        for r in (ring_y[s], ring_z[s]):
            r.far()
            r.near()

    def relay(s):
        ring_y[s].relay()
        ring_z[s].relay()

    def finish(s):
        ring_y[s].finish(put_y(s))
        ring_z[s].finish(put_z(s))

    def begin_second(j):
        second[j].far()
        second[j].near()

    second = [
        Ring4(
            net, y, to_y,
            lambda t, hf: u0.at[t // 2, 2 * hf : 2 * hf + 2, lax.rem(t, 2)], r2.at[0],
        ),
        Ring4(net, z, to_z, lambda t, hf: u1.at[t, 2 * hf : 2 * hf + 2], r2.at[1]),
        Ring4(net, x, to_x, lambda t, hf: u2.at[hf, t], r2.at[2]),
    ]

    def put2(j):
        def put(hf, val):
            v[j, 2 * hf : 2 * hf + 2] = val.astype(BF)

        return put

    last_axis = [(z, to_z), (x, to_x), (y, to_y)]
    last = [None] * 3

    def third(j):
        me, to = last_axis[j]
        last[j] = [net.copy(v.at[j, rem4(me + d)], r3.at[j, d - 1], to(d)) for d in (1, 2, 3)]

    def rs_end(j):
        total = v[j, last_axis[j][0]].astype(F32)
        for d in range(3):
            last[j][d].wait_recv()
            total = total + r3[j, d].astype(F32)
        gh[j] = total.astype(BF)

    def end_second(j):
        second[j].finish(put2(j))
        third(j)

    def weight_grad(n):
        cols = slice(n * 512, (n + 1) * 512)
        hn = h[:, :, :, :, :, cols].reshape(768, 512)
        w[:, cols] = jnp.dot(g[...], hn, preferred_element_type=F32).astype(BF)

    bp = bucket_pair()
    place_meta()
    relay_near(0)
    relay_near(1)
    relay_other(0)
    relay_near(2)
    relay_other(1)
    relay_other(2)
    relay_far(0)
    relay_far(1)
    relay_last(0)
    relay_far(2)
    relay_end(0)
    meta_next(1)
    relay_last(1)
    relay_end(1)
    ld_w.wait()
    ag[0]["d0"].wait_recv()
    logits(0, mine, True)
    relay_last(2)
    relay_end(2)
    bucket_sum(bp)
    bz.far()
    bz.near()
    ag[1]["d0"].wait_recv()
    logits(1, mine, True)
    gather_across(0)
    gather_across(1)
    ag[2]["d0"].wait_recv()
    logits(2, mine, True)
    meta_next(2)
    ag[0]["d1"].wait_recv()
    logits(0, other, False)
    gather_across(2)
    bz.relay()
    ag[1]["d1"].wait_recv()
    logits(1, other, False)
    ag[2]["d1"].wait_recv()
    logits(2, other, False)
    local_stats()
    stats_send(0)
    bz.finish(b_put)
    b_y[...] = b_u[1 - yh].astype(BF)
    stats_next(1)
    stats_next(2)
    stats_end()
    by = net.copy(b_y, b_ry, {"dp_0": 1 - yh})
    grads()
    product(1, xs_of[0], 2)
    cross(0)
    terms(0)
    joined(0)
    ring_x.far()
    start(0)
    terms(1)
    joined(1)
    ring_x.near_plus()
    start(1)
    terms(2)
    relay(0)
    joined(2)
    ring_x.near_minus()
    start(2)
    product(0, xs_of[3], 1)
    ring_x.relay_plus()
    ring_x.relay_minus()
    relay(1)
    joined(3)
    start(3)
    weight_grad(0)
    weight_grad(1)
    relay(2)
    finish(0)
    weight_grad(2)
    finish(1)
    relay(3)
    weight_grad(3)
    weight_grad(4)
    finish(2)
    ring_x.finish(put_x)
    begin_second(0)
    finish(3)
    begin_second(1)
    begin_second(2)
    by.wait_recv()
    rb[...] = (b_u[yh] + b_ry[...].astype(F32)) * factor_of(mt_c[6:7, 0:1])
    weight_grad(5)
    weight_grad(6)
    second[0].relay()
    second[1].relay()
    second[2].relay()
    weight_grad(7)
    end_second(0)
    end_second(1)
    end_second(2)
    weight_grad(8)
    weight_grad(9)
    rs_end(0)
    rs_end(1)
    rs_end(2)
    for cp in net.all:
        cp.wait_send()


def flush(gw_in, gh_in, rb_in, gh, gw, rb, sems):
    copies = [
        pltpu.make_async_copy(gw_in.at[rows], gw.at[rows], sems.at[i])
        for i, rows in enumerate(pl.ds(128 * k, 128) for k in range(8))
    ]
    copies.append(pltpu.make_async_copy(gh_in, gh, sems.at[8]))
    copies.append(pltpu.make_async_copy(rb_in, rb, sems.at[9]))
    for cp in copies:
        cp.start()
    for cp in copies:
        cp.wait()


def on_device(hidden, head_weight, target_ids, response_mask, advantages, seq_tokens, layer_grads):
    vm = pltpu.VMEM
    anywhere = pl.BlockSpec(memory_space=pl.ANY)
    in_vmem = pl.BlockSpec(memory_space=pltpu.VMEM)
    piece = (16, 640)
    scratch = [
        vm((1024, 768), BF),
        vm((3, 2, 2, 4, 16, 5120), BF),
        vm((1024, 768), F32),
        vm((2, 3, 128, 1024), BF),
        vm((6, 2, 3, 2, 4, *piece), BF),
        vm((4, 2, 3, 2, 4, *piece), BF),
        vm((3, 2, 4, 4, 2, *piece), BF),
        vm((2, 3, 4, 2, *piece), BF),
        vm((4, 2, 3, 2, *piece), BF),
        vm((4, 2, 3, 2, *piece), BF),
        vm((2, 4, 2, *piece), BF),
        vm((4, 4, *piece), BF),
        vm((2, 4, 2, *piece), BF),
        vm((3, 2, 3, 2, *piece), BF),
        vm((3, 4, *piece), BF),
        vm((3, 3, *piece), BF),
        vm((3, 8, 384), F32),
        vm((8, 384), F32),
        vm((3, 7, 8, 384), F32),
        vm((8, 768), F32),
        vm((3, 8, 384), F32),
        vm((8, 384), F32),
        vm((3, 3, 8, 384), F32),
        vm((2, 4, 64, 1024), F32),
        vm((2, 4, 64, 1024), F32),
        vm((2, 4, 64, 1024), BF),
        vm((2, 4, 64, 1024), BF),
        vm((2, 4, 64, 1024), BF),
        vm((2, 3, 64, 1024), BF),
        vm((2, 64, 1024), F32),
        vm((64, 1024), BF),
        vm((64, 1024), BF),
        pltpu.SemaphoreType.DMA((COPIES,)),
        pltpu.SemaphoreType.DMA((COPIES,)),
        pltpu.SemaphoreType.DMA((4,)),
    ]
    gw, gh, rb = pl.pallas_call(
        kernel,
        out_shape=(
            vm((1024, 5120), BF),
            vm((3, 16, 640), BF),
            vm((64, 1024), F32),
        ),
        in_specs=[anywhere, anywhere, in_vmem, in_vmem, in_vmem, in_vmem, anywhere],
        out_specs=(in_vmem,) * 3,
        scratch_shapes=scratch,
        compiler_params=pltpu.CompilerParams(
            collective_id=0, has_side_effects=True, vmem_limit_bytes=55 * 1000 * 1000
        ),
    )(
        hidden.reshape(3, 16, 5120),
        head_weight,
        target_ids,
        response_mask,
        advantages,
        seq_tokens,
        layer_grads.reshape(2, 4, 2, 64, 1024),
    )
    gh, gw, rb = pl.pallas_call(
        flush,
        out_shape=(
            jax.ShapeDtypeStruct((3, 16, 640), BF),
            jax.ShapeDtypeStruct((1024, 5120), BF),
            jax.ShapeDtypeStruct((64, 1024), F32),
        ),
        in_specs=[in_vmem] * 3,
        out_specs=(anywhere,) * 3,
        scratch_shapes=[pltpu.SemaphoreType.DMA((10,))],
        compiler_params=pltpu.CompilerParams(vmem_limit_bytes=16 * 1024 * 1024),
    )(gw, gh, rb)
    return gh.reshape(48, 640), gw, rb


def solution(mesh):
    split = Mesh(
        mesh.devices.reshape(2, 4, 2, 4, 2), ("dp_0", "dp_1", "dp_2", "vocab_0", "vocab_1")
    )
    return jax.shard_map(
        on_device,
        mesh=split,
        in_specs=(P(DP, None), P(DP_VOCAB, None), P(DP), P(DP), P(DP), P(DP), P(DP, None, VOCAB)),
        out_specs=(P(DP, VOCAB), P(DP_VOCAB, None), P(DP, VOCAB)),
        check_vma=False,
    )
```

```python
import functools

import jax
import jax.numpy as jnp
from jax import lax
from jax.experimental import pallas as pl
from jax.experimental.pallas import tpu as pltpu
from jax.sharding import Mesh
from jax.sharding import PartitionSpec as P

VOCAB = ("vocab_0", "vocab_1")
DP = ("dp_0", "dp_1", "dp_2")
DP_VOCAB = ("dp_0", "dp_1", "dp_2", "vocab_0", "vocab_1")
BF, F32 = jnp.bfloat16, jnp.float32

loss_scale = 16.0
entropy_coef = 0.1

COPIES = 164
SEND_SLOTS = 72


def rem4(v):
    return lax.rem(v, 4)


class Net:
    def __init__(self, send_sems, recv_sems):
        self.send_sems, self.recv_sems, self.all = send_sems, recv_sems, []
        self.slots, self.free, self.made = [], [], 0

    def copy(self, src, dst, dev):
        i = len(self.all)
        if not self.free:
            self.free.append(self.made)
            self.made += 1
        slot = self.free.pop()
        self.slots.append(slot)
        c = pltpu.make_async_remote_copy(
            src_ref=src,
            dst_ref=dst,
            send_sem=self.send_sems.at[slot],
            recv_sem=self.recv_sems.at[i],
            device_id=dev,
            device_id_type=pl.DeviceIdType.MESH,
        )
        c.start()
        self.all.append(c)
        return c


class Ring4:
    def __init__(self, net, me, to, chunk, recv):
        self.net, self.me, self.to, self.chunk, self.recv = net, me, to, chunk, recv

    def far(self):
        t = rem4(self.me + 2)
        self.c1 = self.net.copy(self.chunk(t, 0), self.recv.at[0, 0], self.to(1))
        self.c2 = self.net.copy(self.chunk(t, 1), self.recv.at[1, 0], self.to(3))

    def near_plus(self):
        self.c3 = self.net.copy(self.chunk(rem4(self.me + 1), 1), self.recv.at[0, 1], self.to(1))

    def near_minus(self):
        self.c4 = self.net.copy(self.chunk(rem4(self.me + 3), 0), self.recv.at[1, 1], self.to(3))

    def near(self):
        self.near_plus()
        self.near_minus()

    def relay_plus(self):
        d = self.chunk(rem4(self.me + 1), 0)
        self.c1.wait_recv()
        d[...] = (d[...].astype(F32) + self.recv[0, 0].astype(F32)).astype(BF)
        self.c5 = self.net.copy(d, self.recv.at[0, 2], self.to(1))

    def relay_minus(self):
        d = self.chunk(rem4(self.me + 3), 1)
        self.c2.wait_recv()
        d[...] = (d[...].astype(F32) + self.recv[1, 0].astype(F32)).astype(BF)
        self.c6 = self.net.copy(d, self.recv.at[1, 2], self.to(3))

    def relay(self):
        self.relay_plus()
        self.relay_minus()

    def finish(self, put):
        for c in (self.c3, self.c4, self.c5, self.c6):
            c.wait_recv()
        r, mine = self.recv, self.chunk
        me = rem4(self.me)
        put(0, mine(me, 0)[...].astype(F32) + r[0, 2].astype(F32) + r[1, 1].astype(F32))
        put(1, mine(me, 1)[...].astype(F32) + r[0, 1].astype(F32) + r[1, 2].astype(F32))


def kernel(
    hid, w_hbm, tgt, msk, adv, seq, lg, w, gh, rb,
    g, h, logit, gt, half, rcv, t_buf, r1, r1y, r1z, u0, u1, u2, r2, v, r3,
    st_s, st_c, st_r, put_at, mt_s, mt_c, mt_r, b_sib, b_own, b_s, b_r, b, b_rz, b_u, b_y, b_ry,
    send_sems, recv_sems, local_sems,
):
    yh, z, c = lax.axis_index("dp_0"), lax.axis_index("dp_1"), lax.axis_index("dp_2")
    x, yl = lax.axis_index("vocab_0"), lax.axis_index("vocab_1")
    y = 2 * yh + yl
    k = lax.rem(x + yh + yl, 2)

    def to_x(d):
        return {"vocab_0": rem4(x + d)}

    def to_z(d):
        return {"dp_1": rem4(z + d)}

    def to_y(d):
        n = rem4(y + d)
        return {"dp_0": n // 2, "vocab_1": lax.rem(n, 2)}

    y_other = {"dp_0": 1 - yh, "vocab_1": 1 - yl}
    y_same = {"vocab_1": 1 - yl}
    core = {"dp_2": 1 - c}

    net = Net(send_sems, recv_sems)

    ld_h = pltpu.make_async_copy(hid, h.at[:, c, yh, z], local_sems.at[0])
    ld_h.start()
    ld_bs = pltpu.make_async_copy(lg.at[:, :, 1 - c], b_sib, local_sems.at[1])
    ld_bs.start()
    ld_w = pltpu.make_async_copy(w_hbm, w, local_sems.at[2])
    ld_w.start()
    ld_bo = pltpu.make_async_copy(lg.at[:, :, c], b_own, local_sems.at[3])
    ld_bo.start()

    barrier = pltpu.get_barrier_semaphore()
    peers = [core] + [f(d) for f in (to_x, to_y, to_z) for d in (1, 3)]
    for p in peers:
        pl.semaphore_signal(barrier, inc=1, device_id=p, device_id_type=pl.DeviceIdType.MESH)
    pl.semaphore_wait(barrier, len(peers))
    ld_h.wait()

    mine = pl.ds(pl.multiple_of(k * 2560, 128), 2560)
    other = pl.ds(pl.multiple_of((1 - k) * 2560, 128), 2560)
    lower = pl.ds(pl.multiple_of(k * 2560, 128), 1280)
    upper = pl.ds(pl.multiple_of(k * 2560 + 1280, 128), 1280)

    def piece(j, hi, zz, cols):
        return h.at[j, c, hi, zz, :, cols]

    def hop(j, hi, zz, cols, dev):
        ref = piece(j, hi, zz, cols)
        return net.copy(ref, ref, dev)

    yo, zm, zp, z2 = 1 - yh, rem4(z + 3), rem4(z + 1), rem4(z + 2)
    sides = (to_x(1), to_x(3), y_same)
    ag = [{} for _ in range(3)]
    for j in range(3):
        ag[j]["zm"] = hop(j, yh, z, mine, to_z(1))
        ag[j]["zp"] = hop(j, yh, z, mine, to_z(3))
        ag[j]["yo"] = hop(j, yh, z, mine, y_other)

    def across(j, p, hi, zz):
        ag[j]["b%d" % p] = hop(j, hi, zz, mine, sides[(p + j) % 3])

    def relay_near(j):
        a = ag[j]
        a["zm"].wait_recv()
        a["z2l"] = hop(j, yh, zm, lower, to_z(1))
        across(j, 0, yh, zm)
        a["zp"].wait_recv()
        a["z2u"] = hop(j, yh, zp, upper, to_z(3))
        across(j, 1, yh, zp)

    def relay_other(j):
        a = ag[j]
        a["yo"].wait_recv()
        a["zmo"] = hop(j, yo, z, mine, to_z(1))
        a["zpo"] = hop(j, yo, z, mine, to_z(3))
        across(j, 2, yo, z)

    def relay_far(j):
        a = ag[j]
        a["z2l"].wait_recv()
        a["z2u"].wait_recv()
        a["yo2"] = hop(j, yh, z2, mine, y_other)
        across(j, 5, yh, z2)

    def relay_last(j):
        a = ag[j]
        a["zmo"].wait_recv()
        across(j, 3, yo, zm)
        a["zpo"].wait_recv()
        across(j, 4, yo, zp)

    def relay_end(j):
        a = ag[j]
        a["yo2"].wait_recv()
        across(j, 6, yo, z2)
        ref = h.at[j, c, :, :, :, mine]
        a["d0"] = net.copy(ref, ref, core)

    def gather_across(j):
        for p in range(7):
            ag[j]["b%d" % p].wait_recv()
        ref = h.at[j, c, :, :, :, other]
        ag[j]["d1"] = net.copy(ref, ref, core)

    def gather_done(j):
        ag[j]["d0"].wait_recv()
        ag[j]["d1"].wait_recv()

    def bucket_pair():
        ld_bs.wait()
        b_s[...] = b_sib[...].astype(BF)
        return net.copy(b_s, b_r, core)

    def bucket_sum(cp):
        ld_bo.wait()
        cp.wait_recv()
        b[...] = (b_own[...] + b_r[...].astype(F32)).astype(BF)

    bz = Ring4(net, z, to_z, lambda t, hf: b.at[hf, t], b_rz)

    def b_put(hf, val):
        b_u[hf] = val

    def logits(j, cols, first):
        def block(i, _):
            rows = pl.ds(pl.multiple_of(i * 512, 512), 512)
            part = lax.dot_general(
                w[rows, cols], h[j, :, :, :, :, cols].reshape(256, 2560),
                (((1,), (1,)), ((), ())), preferred_element_type=F32,
            )
            if not first:
                part = part + logit[rows, j * 256 : (j + 1) * 256]
            logit[rows, j * 256 : (j + 1) * 256] = part
            return 0

        lax.fori_loop(0, 2, block, 0)

    def place_meta():
        r8 = lax.broadcasted_iota(jnp.int32, (8, 48), 0)
        rows = jnp.zeros((8, 48), F32)
        for r, ref in enumerate((tgt, msk, adv)):
            rows = jnp.where(r8 == r, ref[...].astype(F32).reshape(1, 48), rows)
        count = jnp.sum(seq[...].astype(F32).reshape(1, 8), axis=1, keepdims=True)
        token = lax.broadcasted_iota(jnp.int32, (48, 256), 0)
        lane = lax.broadcasted_iota(jnp.int32, (48, 256), 1)
        base = (c * 8 + yh * 4 + z) * 16
        for j in range(3):
            hot = jnp.where(lane - base == token - 16 * j, 1.0, 0.0)
            hot = jnp.where((token >= 16 * j) & (token < 16 * j + 16), hot, 0.0)
            put = lax.dot_general(
                rows, hot, (((1,), (0,)), ((), ())),
                preferred_element_type=F32, precision=lax.Precision.HIGHEST,
            )
            r_id = lax.broadcasted_iota(jnp.int32, (8, 256), 0)
            tile = jnp.where(r_id == 6, count, 0.0)
            for r in range(3):
                tile = jnp.where(r_id == 3 + r, put[r : r + 1], tile)
            put_at[:, j * 256 : (j + 1) * 256] = tile

        pack(mt_s.at[0], [put_at[r : r + 1] for r in (3, 4, 5)])
        mt_s[0, 6:8] = jnp.broadcast_to(count, (2, 384))
        meta_send(0)

    def pack(ref, rows):
        for i, row in enumerate(rows):
            ref[2 * i : 2 * i + 1] = row[:, :384]
            ref[2 * i + 1 : 2 * i + 2] = row[:, 384:]

    def unpack(tile, i):
        return jnp.concatenate([tile[2 * i : 2 * i + 1], tile[2 * i + 1 : 2 * i + 2]], axis=1)

    meta_phases = ([core], [to_y(d) for d in (1, 2, 3)], [to_z(d) for d in (1, 2, 3)])
    mt = {}

    def meta_send(ph):
        mt[ph] = [
            net.copy(mt_s.at[ph], mt_r.at[ph, d], dev) for d, dev in enumerate(meta_phases[ph])
        ]

    def meta_sum(ph):
        total = mt_s[ph]
        for d, cp in enumerate(mt[ph]):
            cp.wait_recv()
            total = total + mt_r[ph, d]
        return total

    def meta_next(ph):
        mt_s[ph] = meta_sum(ph - 1)
        meta_send(ph)

    def local_stats():
        def top(i, m):
            blk = logit[pl.ds(pl.multiple_of(i * 64, 64), 64)]
            return jnp.maximum(m, jnp.max(blk.reshape(8, 8, 768), axis=0))

        m8 = lax.fori_loop(0, 16, top, jnp.full((8, 768), -jnp.inf, F32))
        m = jnp.max(m8, axis=0, keepdims=True)

        def sums(i, se):
            blk = logit[pl.ds(pl.multiple_of(i * 64, 64), 64)]
            e = jnp.exp(blk - m)
            return (
                se[0] + jnp.sum(e.reshape(8, 8, 768), axis=0),
                se[1] + jnp.sum((e * blk).reshape(8, 8, 768), axis=0),
            )

        zero = jnp.zeros((8, 768), F32)
        s8, e8 = lax.fori_loop(0, 16, sums, (zero, zero))
        s = jnp.sum(s8, axis=0, keepdims=True)
        e = jnp.sum(e8, axis=0, keepdims=True)
        pack(st_s.at[0], (m, s, e))
        st_s[0, 6:8] = jnp.zeros((2, 384), F32)

    phases = (
        [core] + [to_x(d) for d in (1, 2, 3)] + [{**core, **to_x(d)} for d in (1, 2, 3)],
        [to_y(d) for d in (1, 2, 3)],
        [to_z(d) for d in (1, 2, 3)],
    )
    st = {}

    def stats_send(ph):
        st[ph] = [net.copy(st_s.at[ph], st_r.at[ph, d], dev) for d, dev in enumerate(phases[ph])]

    def stats_sum(ph, out):
        tiles = [st_s[ph]]
        for d, cp in enumerate(st[ph]):
            cp.wait_recv()
            tiles.append(st_r[ph, d])
        m = functools.reduce(jnp.maximum, [t[0:2] for t in tiles])
        scales = [jnp.exp(t[0:2] - m) for t in tiles]
        out[0:2] = m
        for at in (2, 4):
            out[at : at + 2] = sum(t[at : at + 2] * f for t, f in zip(tiles, scales))
        out[6:8] = jnp.zeros((2, 384), F32)

    def stats_next(ph):
        stats_sum(ph - 1, st_s.at[ph])
        stats_send(ph)

    def stats_end():
        stats_sum(2, st_c)
        mt_c[...] = meta_sum(2)

    def factor_of(count_row):
        return (loss_scale * 768.0) / (count_row / 2.0)

    first_id = ((yh * 8 + z * 2 + c) * 8 + x * 2 + yl) * 1024

    def grads():
        tile = st_c[...]
        m, s, e = (unpack(tile, i) for i in range(3))
        target, mask, adv = (unpack(mt_c[...], i) / 2.0 for i in range(3))
        inv = 1.0 / s
        mean = e * inv
        wt = factor_of(mt_c[6:7, 0:1]) * mask
        wa = wt * adv
        wb = wt * entropy_coef

        def block(i, _):
            rows = pl.ds(pl.multiple_of(i * 128, 128), 128)
            l = logit[rows]
            ids = (first_id + i * 128 + lax.broadcasted_iota(jnp.int32, (128, 768), 0)).astype(F32)
            p = jnp.exp(l - m) * inv
            val = p * (wa + wb * (l - mean))
            val = jnp.where(ids == target, val - wa, val)
            val = val.astype(BF)
            g[rows] = val
            for j in range(3):
                for cc in range(2):
                    at = (2 * j + cc) * 128
                    gt[(c if cc == 0 else 1 - c), j, :, rows] = val[:, at : at + 128].T
            return 0

        lax.fori_loop(0, 8, block, 0)

    xs_of = [rem4(x + 2), rem4(x + 1), rem4(x + 3), x]
    pair = {}

    def product(side, block, slot):
        cols = pl.ds(pl.multiple_of(block * 1280, 128), 1280)
        acc = jnp.dot(gt[side].reshape(384, 1024), w[:, cols], preferred_element_type=F32)
        for lo in range(2):
            part = acc[:, lo * 640 : (lo + 1) * 640]
            half[slot, lo] = part.reshape(3, 2, 4, 16, 640).astype(BF)

    def cross(s):
        pair[s] = net.copy(half.at[2 + s], rcv.at[s], core)

    def terms(s):
        def side(i, _):
            block = xs_of[s] + i * (xs_of[s + 1] - xs_of[s])
            product(i, block, s % 2 + i * (3 + s - s % 2))
            return 0

        lax.fori_loop(0, 2, side, 0)
        cross(s + 1)

    def joined(s):
        pair[s].wait_recv()
        for lo in range(2):
            t_buf[:, :, :, xs_of[s], lo] = (
                half[s % 2, lo].astype(F32) + rcv[s, lo].astype(F32)
            ).astype(BF)

    t0, t1, t2 = t_buf.at[0], t_buf.at[1], t_buf.at[2]
    ring_x = Ring4(net, x, to_x, lambda t, hf: t0.at[hf, :, t], r1)
    ring_y, ring_z = [], []
    for s in range(4):
        ring_y.append(
            Ring4(
                net, y, to_y,
                lambda t, hf, s=s: t1.at[t // 2, 2 * hf : 2 * hf + 2, xs_of[s], lax.rem(t, 2)],
                r1y.at[s],
            )
        )
        ring_z.append(Ring4(net, z, to_z, lambda t, hf, s=s: t2.at[hf, t, xs_of[s]], r1z.at[s]))

    def put_x(hf, val):
        u0[hf] = val.astype(BF)

    def put_y(s):
        def put(hf, val):
            u1[2 * hf : 2 * hf + 2, xs_of[s]] = val.astype(BF)

        return put

    def put_z(s):
        def put(hf, val):
            u2[hf, xs_of[s]] = val.astype(BF)

        return put

    def start(s):
        for r in (ring_y[s], ring_z[s]):
            r.far()
            r.near()

    def relay(s):
        ring_y[s].relay()
        ring_z[s].relay()

    def finish(s):
        ring_y[s].finish(put_y(s))
        ring_z[s].finish(put_z(s))

    def begin_second(j):
        second[j].far()
        second[j].near()

    second = [
        Ring4(
            net, y, to_y,
            lambda t, hf: u0.at[t // 2, 2 * hf : 2 * hf + 2, lax.rem(t, 2)], r2.at[0],
        ),
        Ring4(net, z, to_z, lambda t, hf: u1.at[t, 2 * hf : 2 * hf + 2], r2.at[1]),
        Ring4(net, x, to_x, lambda t, hf: u2.at[hf, t], r2.at[2]),
    ]

    def put2(j):
        def put(hf, val):
            v[j, 2 * hf : 2 * hf + 2] = val.astype(BF)

        return put

    last_axis = [(z, to_z), (x, to_x), (y, to_y)]
    last = [None] * 3

    def third(j):
        me, to = last_axis[j]
        last[j] = [net.copy(v.at[j, rem4(me + d)], r3.at[j, d - 1], to(d)) for d in (1, 2, 3)]

    def rs_end(j):
        total = v[j, last_axis[j][0]].astype(F32)
        for d in range(3):
            last[j][d].wait_recv()
            total = total + r3[j, d].astype(F32)
        gh[j] = total.astype(BF)

    def end_second(j):
        second[j].finish(put2(j))
        third(j)

    def weight_grad(n):
        cols = slice(n * 512, (n + 1) * 512)
        hn = h[:, :, :, :, :, cols].reshape(768, 512)
        w[:, cols] = jnp.dot(g[...], hn, preferred_element_type=F32).astype(BF)

    sent = [0]

    def drain(upto):
        for i in range(sent[0], upto):
            net.all[i].wait_send()
            net.free.append(net.slots[i])
        sent[0] = upto

    bp = bucket_pair()
    place_meta()
    relay_near(0)
    relay_near(1)
    relay_other(0)
    relay_near(2)
    relay_other(1)
    relay_other(2)
    relay_far(0)
    relay_far(1)
    relay_last(0)
    relay_far(2)
    relay_end(0)
    meta_next(1)
    relay_last(1)
    relay_end(1)
    ld_w.wait()
    ag[0]["d0"].wait_recv()
    logits(0, mine, True)
    relay_last(2)
    relay_end(2)
    bucket_sum(bp)
    bz.far()
    bz.near()
    ag[1]["d0"].wait_recv()
    logits(1, mine, True)
    gather_across(0)
    gather_across(1)
    ag[2]["d0"].wait_recv()
    logits(2, mine, True)
    meta_next(2)
    ag[0]["d1"].wait_recv()
    logits(0, other, False)
    gather_across(2)
    bz.relay()
    ag[1]["d1"].wait_recv()
    logits(1, other, False)
    ag[2]["d1"].wait_recv()
    logits(2, other, False)
    local_stats()
    gathered = len(net.all)
    stats_send(0)
    bz.finish(b_put)
    drain(gathered)
    b_y[...] = b_u[1 - yh].astype(BF)
    stats_next(1)
    stats_next(2)
    stats_end()
    by = net.copy(b_y, b_ry, {"dp_0": 1 - yh})
    grads()
    drain(len(net.all) - 1)
    product(1, xs_of[0], 2)
    cross(0)
    terms(0)
    joined(0)
    ring_x.far()
    start(0)
    terms(1)
    joined(1)
    ring_x.near_plus()
    start(1)
    terms(2)
    relay(0)
    joined(2)
    ring_x.near_minus()
    start(2)
    product(0, xs_of[3], 1)
    ring_x.relay_plus()
    ring_x.relay_minus()
    relay(1)
    joined(3)
    start(3)
    weight_grad(0)
    weight_grad(1)
    relay(2)
    finish(0)
    weight_grad(2)
    finish(1)
    relay(3)
    weight_grad(3)
    weight_grad(4)
    finish(2)
    ring_x.finish(put_x)
    begin_second(0)
    finish(3)
    begin_second(1)
    begin_second(2)
    by.wait_recv()
    rb[...] = (b_u[yh] + b_ry[...].astype(F32)) * factor_of(mt_c[6:7, 0:1])
    weight_grad(5)
    drain(len(net.all) - 30)
    weight_grad(6)
    second[0].relay()
    second[1].relay()
    second[2].relay()
    weight_grad(7)
    end_second(0)
    end_second(1)
    end_second(2)
    weight_grad(8)
    drain(len(net.all) - 9)
    weight_grad(9)
    rs_end(0)
    rs_end(1)
    rs_end(2)
    drain(len(net.all))


def flush(gw_in, gh_in, rb_in, gh, gw, rb, sems):
    copies = [
        pltpu.make_async_copy(gw_in.at[rows], gw.at[rows], sems.at[i])
        for i, rows in enumerate(pl.ds(128 * k, 128) for k in range(8))
    ]
    copies.append(pltpu.make_async_copy(gh_in, gh, sems.at[8]))
    copies.append(pltpu.make_async_copy(rb_in, rb, sems.at[9]))
    for cp in copies:
        cp.start()
    for cp in copies:
        cp.wait()


def on_device(hidden, head_weight, target_ids, response_mask, advantages, seq_tokens, layer_grads):
    vm = pltpu.VMEM
    anywhere = pl.BlockSpec(memory_space=pl.ANY)
    in_vmem = pl.BlockSpec(memory_space=pltpu.VMEM)
    piece = (16, 640)
    scratch = [
        vm((1024, 768), BF),
        vm((3, 2, 2, 4, 16, 5120), BF),
        vm((1024, 768), F32),
        vm((2, 3, 128, 1024), BF),
        vm((6, 2, 3, 2, 4, *piece), BF),
        vm((4, 2, 3, 2, 4, *piece), BF),
        vm((3, 2, 4, 4, 2, *piece), BF),
        vm((2, 3, 4, 2, *piece), BF),
        vm((4, 2, 3, 2, *piece), BF),
        vm((4, 2, 3, 2, *piece), BF),
        vm((2, 4, 2, *piece), BF),
        vm((4, 4, *piece), BF),
        vm((2, 4, 2, *piece), BF),
        vm((3, 2, 3, 2, *piece), BF),
        vm((3, 4, *piece), BF),
        vm((3, 3, *piece), BF),
        vm((3, 8, 384), F32),
        vm((8, 384), F32),
        vm((3, 7, 8, 384), F32),
        vm((8, 768), F32),
        vm((3, 8, 384), F32),
        vm((8, 384), F32),
        vm((3, 3, 8, 384), F32),
        vm((2, 4, 64, 1024), F32),
        vm((2, 4, 64, 1024), F32),
        vm((2, 4, 64, 1024), BF),
        vm((2, 4, 64, 1024), BF),
        vm((2, 4, 64, 1024), BF),
        vm((2, 3, 64, 1024), BF),
        vm((2, 64, 1024), F32),
        vm((64, 1024), BF),
        vm((64, 1024), BF),
        pltpu.SemaphoreType.DMA((SEND_SLOTS,)),
        pltpu.SemaphoreType.DMA((COPIES,)),
        pltpu.SemaphoreType.DMA((4,)),
    ]
    gw, gh, rb = pl.pallas_call(
        kernel,
        out_shape=(
            vm((1024, 5120), BF),
            vm((3, 16, 640), BF),
            vm((64, 1024), F32),
        ),
        in_specs=[anywhere, anywhere, in_vmem, in_vmem, in_vmem, in_vmem, anywhere],
        out_specs=(in_vmem,) * 3,
        scratch_shapes=scratch,
        compiler_params=pltpu.CompilerParams(
            collective_id=0, has_side_effects=True, vmem_limit_bytes=55 * 1000 * 1000
        ),
    )(
        hidden.reshape(3, 16, 5120),
        head_weight,
        target_ids,
        response_mask,
        advantages,
        seq_tokens,
        layer_grads.reshape(2, 4, 2, 64, 1024),
    )
    gh, gw, rb = pl.pallas_call(
        flush,
        out_shape=(
            jax.ShapeDtypeStruct((3, 16, 640), BF),
            jax.ShapeDtypeStruct((1024, 5120), BF),
            jax.ShapeDtypeStruct((64, 1024), F32),
        ),
        in_specs=[in_vmem] * 3,
        out_specs=(anywhere,) * 3,
        scratch_shapes=[pltpu.SemaphoreType.DMA((10,))],
        compiler_params=pltpu.CompilerParams(vmem_limit_bytes=16 * 1024 * 1024),
    )(gw, gh, rb)
    return gh.reshape(48, 640), gw, rb


def solution(mesh):
    split = Mesh(
        mesh.devices.reshape(2, 4, 2, 4, 2), ("dp_0", "dp_1", "dp_2", "vocab_0", "vocab_1")
    )
    return jax.shard_map(
        on_device,
        mesh=split,
        in_specs=(P(DP, None), P(DP_VOCAB, None), P(DP), P(DP), P(DP), P(DP), P(DP, None, VOCAB)),
        out_specs=(P(DP, VOCAB), P(DP_VOCAB, None), P(DP, VOCAB)),
        check_vma=False,
    )
```
